512 devices in a mesh: elem: 128 (over z, x_lo, y), chan: 4 (over x_hi, core).
Axes of the slice: x: 4 (x_hi: 2, x_lo: 2; x = x_hi * 2 + x_lo), y: 8, z: 8, core: 2. Of those that a mesh axis runs over, the one named last changes fastest.
Arguments:
- voltages: bfloat16 [2, 16384, 19584], P(None, ('elem', 'chan')), may hold values from -6 to 6
- delays: int32 [16384], P(('elem', 'chan')), may hold values from 0 to 127
- prototype: bfloat16 [16, 1024], replicated, may hold values from -1.5 to 1.5
- subband_map: int32 [16], replicated, may hold values from 0 to 1023, as said below
- beam_weights: bfloat16 [512, 2, 16, 16384], P('elem', None, 'chan'), may hold values from -0.1875 to 0.1875
Outputs:
- element_power: bfloat16 [16384, 1024], P(('elem', 'chan'))
- beam_voltages: float32 [2, 64, 512], P(None, 'chan', 'elem')
The draws below stay inside these ranges and needn't reach their ends.
Inputs may be any that keep to these rules, and one draw needn't show every extreme that they name: `subband_map`: distinct channel numbers.
All inputs are finite; a program needn't handle non-finite values.
Results may differ from the reference program's by a relative error of at most 0.007.
Values may be sent and summed in bfloat16 or wider, within the bound.
A program may use at most 128 MiB of HBM per device.

```python
import math
import jax
import jax.numpy as jnp
from jax import lax

CH = 1024
TAPS = 16
BEAMS = 512
E_DEV = 32
FRAMES = 4
MAXD = 128
ELEMS = 16384
SUB = 16
SAMP = 19584


def draw_subband_map(key, part):
    return jax.random.permutation(key, CH)[:SUB].astype(jnp.int32)


def plant(values, rng, smallest, top_value):
    extent = values.shape
    index_at = [jax.random.randint(jax.random.fold_in(rng, axis), (), 0, extent[axis]) for axis in range(len(extent))]
    values = values.at[tuple(index_at)].set(smallest)
    longest = extent.index(max(extent))
    index_at[longest] = (index_at[longest] + 1) % extent[longest]
    return values.at[tuple(index_at)].set(top_value)


def with_spikes(result, key, source, target, parts, factor):
    def block_of(position):
        return (jnp.arange(result.shape[position]) // (result.shape[position] // parts)).reshape((-1,) + (1,) * (result.ndim - 1 - position))

    near = jax.random.permutation(key, parts)[block_of(target)]
    other_side = (block_of(target) + parts // 2) % parts
    return jnp.where((block_of(source) == near) | (block_of(source) == other_side), factor * result, result)


def block_levels(key, extent, split, least, high):
    def one(axis_at, blocks):
        draws = jax.random.uniform(jax.random.fold_in(jax.random.fold_in(key, 6), axis_at), (blocks,), jnp.float32, least / len(split), high / len(split))
        return jnp.repeat(jnp.exp(draws), extent[axis_at] // blocks).reshape((-1,) + (1,) * (len(extent) - axis_at - 1))

    gain = one(*split[0])
    for cut in split[1:]:
        gain = gain * one(*cut)
    return gain


def normal_values(stream_key, extent, scale, limit, shards=(), held_as=jnp.bfloat16):
    entries = scale * jax.random.normal(stream_key, extent, jnp.float32)
    if shards:
        entries = entries * block_levels(stream_key, extent, shards, -0.22, 0.18)
    return jnp.clip(entries, -limit, limit).astype(held_as)


def bell_draw_with(own_key, dims, spread, bound, split, heavy, kind=jnp.bfloat16):
    drawn = spread * jax.random.normal(own_key, dims, jnp.float32)
    if split:
        drawn = drawn * block_levels(own_key, dims, split, -0.22, 0.18)
    return jnp.clip(with_spikes(drawn, jax.random.fold_in(own_key, 3), *heavy), -bound, bound).astype(kind)


def setup_inputs(seed: int = 0) -> dict:
    seeds = jax.random.split(jax.random.key(seed), 6)
    voltages = normal_values(seeds[0], (2, ELEMS, SAMP), 1.0, 6.0, ((1, 512),))
    delays = plant(jax.random.randint(seeds[1], (ELEMS,), 0, MAXD), jax.random.fold_in(seeds[1], 1), 0, MAXD - 1).astype(jnp.int32)
    prototype = normal_values(seeds[2], (TAPS, CH), 0.25, 1.5)
    subband_map = draw_subband_map(jax.random.fold_in(seeds[5], 71), 0)
    beam_weights = bell_draw_with(seeds[4], (BEAMS, 2, SUB, ELEMS), ELEMS ** -0.5, 0.1875, ((0, 128), (2, 4)), (3, 0, 128, 5.5))
    return {"voltages": voltages, "delays": delays, "prototype": prototype, "subband_map": subband_map, "beam_weights": beam_weights}


def filtered(voltages, delays, prototype):
    tap_count, chan_count = prototype.shape
    blocks = FRAMES + tap_count - 1
    window_len = blocks * chan_count

    def window(samples, offset):
        return lax.dynamic_slice_in_dim(samples, offset, window_len, 0)
    segments = jax.vmap(jax.vmap(window, in_axes=(0, 0)), in_axes=(0, None))(voltages, delays.astype(jnp.int32))
    segments = segments.reshape(voltages.shape[0], voltages.shape[1], blocks, chan_count)
    coeffs = prototype.astype(jnp.float32)
    running = jnp.zeros((voltages.shape[0], voltages.shape[1], FRAMES, chan_count), jnp.float32)
    for tap_index in range(tap_count):
        running = running + coeffs[tap_index] * segments[:, :, tap_index:tap_index + FRAMES, :].astype(jnp.float32)
    return running.astype(jnp.bfloat16)

def reference(voltages, delays, prototype, subband_map, beam_weights):
    groups = ELEMS // E_DEV

    def one_group(number):
        first_elem = number * E_DEV
        voltage_block = lax.dynamic_slice_in_dim(voltages, first_elem, E_DEV, 1)
        shifts = lax.dynamic_slice_in_dim(delays, first_elem, E_DEV, 0)
        filtered_wave = filtered(voltage_block, shifts, prototype)
        signal = filtered_wave[0].astype(jnp.float32) + 1j * filtered_wave[1].astype(jnp.float32)
        spectrum = jnp.fft.fft(signal, axis=-1) / math.sqrt(CH)
        spec_real = jnp.real(spectrum)
        spec_imag = jnp.imag(spectrum)
        power_block = lax.optimization_barrier(jnp.mean(spec_real * spec_real + spec_imag * spec_imag, axis=1)).astype(jnp.bfloat16)
        chosen = jnp.stack([spec_real[:, :, subband_map], spec_imag[:, :, subband_map]]).astype(jnp.bfloat16)
        return (power_block, chosen)
    power_all, chosen_groups = lax.map(one_group, jnp.arange(groups, dtype=jnp.int32))
    element_power = power_all.reshape(ELEMS, CH)
    chosen_all = jnp.transpose(chosen_groups, (1, 4, 3, 0, 2)).reshape(2, SUB, FRAMES, ELEMS)

    def one_subband(number):
        weight_slice = lax.dynamic_index_in_dim(beam_weights, number, 2, keepdims=False)
        spec_slice = lax.dynamic_index_in_dim(chosen_all, number, 1, keepdims=False)

        def contract(spectral, weighting):
            return jnp.dot(spectral, weighting.T, preferred_element_type=jnp.float32)
        out_real = contract(spec_slice[0], weight_slice[:, 0]) - contract(spec_slice[1], weight_slice[:, 1])
        out_imag = contract(spec_slice[1], weight_slice[:, 0]) + contract(spec_slice[0], weight_slice[:, 1])
        return jnp.stack([out_real, out_imag])
    stacked = lax.map(one_subband, jnp.arange(SUB, dtype=jnp.int32))
    beam_voltages = jnp.transpose(stacked, (1, 0, 2, 3)).reshape(2, SUB * FRAMES, BEAMS)
    return (element_power, beam_voltages)
```

```python
import functools
import math

import numpy as np
import jax
import jax.numpy as jnp
from jax import lax
from jax.experimental import pallas as pl
from jax.experimental.pallas import tpu as pltpu
from jax.sharding import Mesh
from jax.sharding import PartitionSpec as P

MESH = pl.DeviceIdType.MESH
CH, TAPS, FRAMES, E_DEV = 1024, 16, 4, 32
BLOCKS = FRAMES + TAPS - 1
SAMP = 19584
RING = 8
LINE = 8
PAD = 40
ORDER = (0, 1, 7, 2, 6, 3, 5, 4)
F32, BF16 = jnp.float32, jnp.bfloat16


def dft_blocks():
    k1 = np.arange(8)[:, None, None]
    p2 = np.arange(128)[None, :, None]
    k2 = np.arange(128)[None, None, :]
    angle = ((p2 * (k1 + 8 * k2)) % CH) * (2.0 * np.pi / CH)
    c, s = np.cos(angle), np.sin(angle)
    top = np.concatenate([c, -s], axis=2)
    low = np.concatenate([s, c], axis=2)
    return np.concatenate([top, low], axis=1).astype(jnp.bfloat16)


def iota(shape, dim):
    return lax.broadcasted_iota(jnp.int32, shape, dim)


def cos_turns(u):
    h = (u - jnp.round(u)) * math.pi
    q = h * h
    s = h * (1.0 + q * (-1.0 / 6 + q * (1.0 / 120 + q * (-1.0 / 5040 + q * (1.0 / 362880 - q * (1.0 / 39916800))))))
    return 1.0 - 2.0 * s * s


def nt_dot(a, b):
    return lax.dot_general(a, b, (((1,), (1,)), ((), ())), preferred_element_type=F32)


def rotated_taps(delay_s, proto_v, taps_a, taps_b, coef):
    taps = proto_v[...].astype(F32)
    for j in range(8):
        block = taps[:, 128 * j : 128 * j + 128]
        taps_a[pl.ds(j, TAPS, stride=8), :] = block
        taps_b[pl.ds((j + 1) % 8, TAPS, stride=8), :] = block
    lane = iota((128, 128), 1)

    def one(n, carry):
        d = delay_s[n]
        mixed = jnp.where(lane < 128 - d, taps_a[...], taps_b[...])
        coef[pl.ds(n, 128, stride=PAD), :] = pltpu.roll(mixed, d, 1)
        return carry

    lax.fori_loop(0, E_DEV, one, 0)


def delay_column(delay_s, column):
    row = iota((E_DEV, 128), 0)
    value = jnp.zeros((E_DEV, 128), jnp.int32)
    for n in range(E_DEV):
        value = jnp.where(row == n, delay_s[n], value)
    column[...] = value


def channel_rows(map_s, rows):
    row = iota((rows, 128), 0)
    which = ((row // 8) % 4) * 4 + row % 4
    value = jnp.zeros((rows, 128), jnp.int32)
    for s in range(16):
        value = jnp.where(which == s, map_s[s], value)
    return value.astype(F32)


def chosen_basis(map_s, basis):
    chan = channel_rows(map_s, 64) * (1.0 / CH)
    row = iota((64, 128), 0)
    swapped, second = row // 32, (row // 4) % 2
    zero = jnp.zeros((64, 128), F32)
    first_half = jnp.where(swapped == 0, jnp.where(second == 0, zero, 0.25), jnp.where(second == 0, -0.25, zero))
    last_half = jnp.where(swapped == 0, jnp.where(second == 0, -0.25, zero), jnp.where(second == 0, 0.5 + zero, -0.25))
    lane = iota((64, 128), 1)
    for j in range(8):
        turns = chan * (lane + 128 * j).astype(F32)
        basis[:, 128 * j : 128 * j + 128] = cos_turns(turns + first_half).astype(BF16)
        basis[:, CH + 128 * j : CH + 128 * j + 128] = cos_turns(turns + last_half).astype(BF16)


def filter_block(part, g, j, special, volt, coef, column, wave):
    rows = slice(16 * g, 16 * g + 16)

    def samples(b):
        start = b * CH + 128 * j
        if not isinstance(j, int):
            start = pl.multiple_of(start, 128)
        return volt[part, rows, pl.ds(start, 128)].astype(F32)

    sums = [None] * FRAMES
    if special:
        late = iota((16, 128), 1) < column[rows, :]
        following = samples(0)
    taps = {}
    for b in range(BLOCKS):
        if special:
            now = following
            following = samples(b + 1)
            value = jnp.where(late, following, now)
        else:
            value = samples(b)
        if b < TAPS:
            start = (b * 8 + j) * PAD + 16 * g
            if not isinstance(j, int):
                start = pl.multiple_of(start, 8)
            taps[b] = coef[pl.ds(start, 16), :]
        for f in range(FRAMES):
            t = b - f
            if 0 <= t < TAPS:
                term = taps[t] * value
                sums[f] = term if sums[f] is None else sums[f] + term
    column_start = part * CH + 128 * j
    if not isinstance(j, int):
        column_start = pl.multiple_of(column_start, 128)
    for f in range(FRAMES):
        wave[pl.ds(f * E_DEV + 16 * g, 16), pl.ds(column_start, 128)] = sums[f].astype(BF16)


def filter_chunk(part, g, volt, coef, column, wave):
    filter_block(part, g, 0, True, volt, coef, column, wave)

    def one(j, carry):
        filter_block(part, g, j, False, volt, coef, column, wave)
        return carry

    lax.fori_loop(1, 8, one, 0)


def chosen_spectra(delay_s, map_s, basis, wave, chosen):
    both = nt_dot(basis[...], wave[...])
    lane = iota((32, 128), 1) % E_DEV
    delay = jnp.zeros((32, 128), jnp.int32)
    for n in range(E_DEV):
        delay = jnp.where(lane == n, delay_s[n], delay)
    turns = channel_rows(map_s, 32) * delay.astype(F32) * (1.0 / CH)
    picked = both[:32] * cos_turns(turns) + both[32:] * cos_turns(turns - 0.25)
    picked = picked * (1.0 / math.sqrt(CH))
    for c in range(4):
        chosen[c] = picked[8 * c : 8 * c + 8].astype(BF16)


def butterflies(wave, halves):
    root = math.sqrt(0.5)

    def one(i, carry):
        rows = pl.ds(pl.multiple_of(16 * i, 16), 16)
        re = [wave[rows, 128 * j : 128 * j + 128].astype(F32) for j in range(8)]
        im = [wave[rows, CH + 128 * j : CH + 128 * j + 128].astype(F32) for j in range(8)]

        def four(ids):
            a, b, c, d = ids
            pr, pi, qr, qi = re[a] + re[c], im[a] + im[c], re[a] - re[c], im[a] - im[c]
            sr, si, tr, ti = re[b] + re[d], im[b] + im[d], re[b] - re[d], im[b] - im[d]
            return [(pr + sr, pi + si), (qr + ti, qi - tr), (pr - sr, pi - si), (qr - ti, qi + tr)]

        even, odd = four((0, 2, 4, 6)), four((1, 3, 5, 7))
        o1 = ((odd[1][0] + odd[1][1]) * root, (odd[1][1] - odd[1][0]) * root)
        o2 = (odd[2][1], -odd[2][0])
        o3 = ((odd[3][1] - odd[3][0]) * root, -(odd[3][0] + odd[3][1]) * root)
        turned = [odd[0], o1, o2, o3]
        for k in range(4):
            for sign in (0, 1):
                zr = even[k][0] - turned[k][0] if sign else even[k][0] + turned[k][0]
                zi = even[k][1] - turned[k][1] if sign else even[k][1] + turned[k][1]
                halves[k + 4 * sign, rows, 0:128] = zr.astype(BF16)
                halves[k + 4 * sign, rows, 128:256] = zi.astype(BF16)
        return carry

    lax.fori_loop(0, 8, one, 0)


def powers(halves, dft, power_k, power):
    def one(k, carry):
        spec = jnp.dot(halves[k], dft[k], preferred_element_type=F32)
        square = spec * spec
        total = square[:, 0:128] + square[:, 128:256]
        mean = total[0:32] + total[32:64] + total[64:96] + total[96:128]
        mean = mean * (1.0 / (FRAMES * CH))
        power_k[:, pl.ds(pl.multiple_of(128 * k, 128), 128)] = mean.astype(BF16)
        return carry

    lax.fori_loop(0, 8, one, 0)
    source = iota((CH, 128), 0)
    target = source // 128 + 8 * (source % 128)

    def put(m, carry):
        select = jnp.where(target == iota((CH, 128), 1) + 128 * m, 1.0, 0.0).astype(BF16)
        block = jnp.dot(power_k[...], select, preferred_element_type=F32)
        power[:, pl.ds(pl.multiple_of(128 * m, 128), 128)] = block.astype(BF16)
        return carry

    lax.fori_loop(0, 8, put, 0)


def stack_weights(raw, rows_f32, weights):
    def one(i, carry):
        lanes = pl.ds(pl.multiple_of(512 * i, 512), 512)
        for k in range(8):
            rows_f32[4 * k : 4 * k + 4, :] = raw[k, :, lanes].astype(F32)
        weights[:, lanes] = rows_f32[...].astype(BF16)
        return carry

    lax.fori_loop(0, 32, one, 0)


def regroup(arrived, x, out):
    lane = iota((8, 128), 1) // E_DEV
    blocks = [arrived[4 * x + c].astype(F32) for c in range(4)]
    frames = []
    for f in range(FRAMES):
        value = None
        for c in range(4):
            shift = ((c - f) % 4) * E_DEV
            moved = pltpu.roll(blocks[c], shift, 1) if shift else blocks[c]
            value = moved if value is None else jnp.where(lane == c, moved, value)
        frames.append(value)
    out[...] = jnp.concatenate(frames, axis=0).astype(BF16)


def kernel(
    volt_h, delay_h, proto_h, map_h, raw_h, dft_h,
    power_h, beams,
    volt, delay_s, map_s, proto_v, taps_a, taps_b, coef, column, basis, wave, chosen, arrived,
    halves, dft, power_k, power, raw, rows_f32, weights, across_a, across_b, total,
    in_sem, volt_sem, out_sem, x_send, x_recv, one_send, one_recv, two_send, two_recv,
):
    z, xl, y = lax.axis_index("z"), lax.axis_index("xl"), lax.axis_index("y")
    xh, core = lax.axis_index("xh"), lax.axis_index("core")
    line = xl * 4 + xh * 2 + core

    def on_line(r):
        other = lax.rem(line + r, LINE)
        return {"xl": other // 4, "xh": lax.rem(other // 2, 2), "core": lax.rem(other, 2)}

    def on_y(r):
        return {"y": lax.rem(y + r, RING)}

    def on_z(r):
        return {"z": lax.rem(z + r, RING)}

    small = [
        pltpu.make_async_copy(delay_h, delay_s, in_sem.at[0]),
        pltpu.make_async_copy(map_h, map_s, in_sem.at[1]),
        pltpu.make_async_copy(proto_h, proto_v, in_sem.at[2]),
    ]
    for copy in small:
        copy.start()
    chunks = []
    for g in range(2):
        for part in range(2):
            rows = pl.ds(16 * g, 16)
            chunks.append(
                pltpu.make_async_copy(volt_h.at[part, rows, :], volt.at[part, rows, :], volt_sem.at[2 * g + part])
            )
    for copy in chunks:
        copy.start()
    later = [
        pltpu.make_async_copy(raw_h, raw, in_sem.at[3]),
        pltpu.make_async_copy(dft_h, dft, in_sem.at[4]),
    ]
    for copy in later:
        copy.start()

    barrier = pltpu.get_barrier_semaphore()
    for r in range(1, LINE):
        pl.semaphore_signal(barrier, inc=1, device_id=on_line(r), device_id_type=MESH)
    for r in range(1, RING):
        pl.semaphore_signal(barrier, inc=1, device_id=on_y(r), device_id_type=MESH)
        pl.semaphore_signal(barrier, inc=1, device_id=on_z(r), device_id_type=MESH)

    for copy in small:
        copy.wait()
    delay_column(delay_s, column)
    rotated_taps(delay_s, proto_v, taps_a, taps_b, coef)
    chosen_basis(map_s, basis)
    for g in range(2):
        for part in range(2):
            chunks[2 * g + part].wait()
            filter_chunk(part, g, volt, coef, column, wave)
    chosen_spectra(delay_s, map_s, basis, wave, chosen)

    pl.semaphore_wait(barrier, LINE - 1 + 2 * (RING - 1))

    x_copies = []
    for r in range(1, LINE):
        other = lax.rem(line + r, LINE)
        copy = pltpu.make_async_remote_copy(
            src_ref=chosen.at[lax.rem(other, 4)],
            dst_ref=arrived.at[line],
            send_sem=x_send.at[r],
            recv_sem=x_recv.at[r],
            device_id=on_line(r),
            device_id_type=MESH,
        )
        copy.start()
        x_copies.append(copy)
    arrived[line] = chosen[lax.rem(line, 4)]

    later[0].wait()
    stack_weights(raw, rows_f32, weights)

    for copy in x_copies:
        copy.wait_recv()
    regroup(arrived, 0, across_a.at[0, 0])
    regroup(arrived, 1, across_b.at[0, 0])

    across = (across_a, across_b)
    first, second = (on_y, on_z), (on_z, on_y)
    ones = {}
    for i in (7, 6, 5, 4, 3, 2, 1):
        r = ORDER[i]
        for colour in range(2):
            copy = pltpu.make_async_remote_copy(
                src_ref=across[colour].at[0, 0],
                dst_ref=across[colour].at[0, r],
                send_sem=one_send.at[colour, r],
                recv_sem=one_recv.at[colour, r],
                device_id=first[colour](r),
                device_id_type=MESH,
            )
            copy.start()
            ones[colour, r] = copy

    later[1].wait()
    butterflies(wave, halves)
    powers(halves, dft, power_k, power)
    power_out = pltpu.make_async_copy(power, power_h, out_sem)
    power_out.start()

    twos = []

    def forward(colour, way, step, i):
        r = ORDER[i]
        held = step if way == 0 else (RING - step) % RING
        given = step + 1 if way == 0 else RING - step - 1
        copy = pltpu.make_async_remote_copy(
            src_ref=across[colour].at[held, r],
            dst_ref=across[colour].at[given, r],
            send_sem=two_send.at[colour, way, step, r],
            recv_sem=two_recv.at[colour, way, step, r],
            device_id=second[colour](1 if way == 0 else RING - 1),
            device_id_type=MESH,
        )
        copy.start()
        twos.append(copy)
        return copy

    def carries(way, step, i):
        if step < 3:
            return True
        return (i % 2 == way) if step == 3 else False

    total[...] = jnp.zeros_like(total)

    def add(pieces):
        data, weight = [], []
        for colour, held, r in pieces:
            zz = lax.rem(z + RING - (held if colour == 0 else r), RING)
            yy = lax.rem(y + RING - (r if colour == 0 else held), RING)
            block = (zz * 2 + colour) * RING + yy
            data.append(across[colour][held, r])
            weight.append(weights[:, pl.ds(pl.multiple_of(block * 128, 128), 128)])
        total[:, 0:32] += nt_dot(jnp.concatenate(data, axis=1), jnp.concatenate(weight, axis=1))

    flying = {}
    for pair in range(4):
        pieces = []
        for i in (2 * pair, 2 * pair + 1):
            for colour in range(2):
                if i:
                    ones[colour, ORDER[i]].wait_recv()
                for way in range(2):
                    flying[colour, way, 0, i] = forward(colour, way, 0, i)
                pieces.append((colour, 0, ORDER[i]))
        add(pieces)
    for step in range(4):
        for pair in range(4):
            pieces = []
            for i in (2 * pair, 2 * pair + 1):
                for colour in range(2):
                    for way in range(2):
                        if not carries(way, step, i):
                            continue
                        flying[colour, way, step, i].wait_recv()
                        if carries(way, step + 1, i):
                            flying[colour, way, step + 1, i] = forward(colour, way, step + 1, i)
                        pieces.append((colour, step + 1 if way == 0 else RING - step - 1, ORDER[i]))
            add(pieces)

    row, col = iota((32, 128), 0), iota((32, 128), 1)
    same = jnp.where((row % 4 == col % 4) & (col < 32), total[...], 0.0)
    folded = same + pltpu.roll(same, 127, 1) + pltpu.roll(same, 126, 1) + pltpu.roll(same, 125, 1)
    wide = folded.reshape(4, 8, 128)
    crossed = pltpu.roll(pltpu.roll(folded, 124, 1).reshape(4, 8, 128), 4, 1)
    real = iota((4, 8, 128), 1) < 4
    beams[...] = jnp.where(real, wide - crossed, wide + crossed).reshape(32, 128)

    for copy in x_copies:
        copy.wait_send()
    for copy in ones.values():
        copy.wait_send()
    for copy in twos:
        copy.wait_send()
    power_out.wait()


def on_device(voltages, delays, prototype, subband_map, beam_weights):
    raw = beam_weights.reshape(8, 4, 16384)
    dft = jnp.asarray(dft_blocks())
    any_spec = pl.BlockSpec(memory_space=pl.ANY)
    dma = pltpu.SemaphoreType.DMA
    power, beams = pl.pallas_call(
        kernel,
        out_shape=(
            jax.ShapeDtypeStruct((E_DEV, CH), BF16),
            jax.ShapeDtypeStruct((32, 128), F32),
        ),
        in_specs=[any_spec] * 6,
        out_specs=(any_spec, pl.BlockSpec(memory_space=pltpu.VMEM)),
        scratch_shapes=[
            pltpu.VMEM((2, E_DEV, SAMP), BF16),
            pltpu.SMEM((E_DEV,), jnp.int32),
            pltpu.SMEM((16,), jnp.int32),
            pltpu.VMEM((TAPS, CH), BF16),
            pltpu.VMEM((128, 128), F32),
            pltpu.VMEM((128, 128), F32),
            pltpu.VMEM((128 * PAD, 128), F32),
            pltpu.VMEM((E_DEV, 128), jnp.int32),
            pltpu.VMEM((64, 2 * CH), BF16),
            pltpu.VMEM((128, 2 * CH), BF16),
            pltpu.VMEM((4, 8, 128), BF16),
            pltpu.VMEM((8, 8, 128), BF16),
            pltpu.VMEM((8, 128, 256), BF16),
            pltpu.VMEM((8, 256, 256), BF16),
            pltpu.VMEM((E_DEV, CH), BF16),
            pltpu.VMEM((E_DEV, CH), BF16),
            pltpu.VMEM((8, 4, 16384), BF16),
            pltpu.VMEM((32, 512), F32),
            pltpu.VMEM((32, 16384), BF16),
            pltpu.VMEM((RING, RING, 32, 128), BF16),
            pltpu.VMEM((RING, RING, 32, 128), BF16),
            pltpu.VMEM((32, 128), F32),
            dma((5,)),
            dma((4,)),
            dma,
            dma((LINE,)),
            dma((LINE,)),
            dma((2, RING)),
            dma((2, RING)),
            dma((2, 2, 4, RING)),
            dma((2, 2, 4, RING)),
        ],
        compiler_params=pltpu.CompilerParams(collective_id=0, has_side_effects=True),
        name="channelize_and_beamform",
    )(voltages, delays, prototype, subband_map, raw, dft)
    beams = beams.reshape(4, 2, 4, 128)[:, :, :, 0:32:8]
    beams = jnp.transpose(beams, (1, 2, 0, 3)).reshape(2, 16, 4)
    return power, beams


def solution(mesh):
    finer = Mesh(mesh.devices.reshape(8, 2, 8, 2, 2), ("z", "xl", "y", "xh", "core"))
    elem, chan = ("z", "xl", "y"), ("xh", "core")
    placed = (P(None, elem + chan, None), P(elem + chan), P(), P(), P(elem, None, chan, None))
    return jax.shard_map(
        on_device,
        mesh=finer,
        in_specs=placed,
        out_specs=(P(elem + chan, None), P(None, chan, elem)),
        check_vma=False,
    )
```

```python
import functools
import math

import numpy as np
import jax
import jax.numpy as jnp
from jax import lax
from jax.experimental import pallas as pl
from jax.experimental.pallas import tpu as pltpu
from jax.sharding import Mesh
from jax.sharding import PartitionSpec as P

MESH = pl.DeviceIdType.MESH
CH, TAPS, FRAMES, E_DEV = 1024, 16, 4, 32
BLOCKS = FRAMES + TAPS - 1
SAMP = 19584
RING = 8
LINE = 8
PAD = 40
ORDER = (0, 1, 7, 2, 6, 3, 5, 4)
F32, BF16 = jnp.float32, jnp.bfloat16


def dft_blocks():
    k1 = np.arange(8)[:, None, None]
    p2 = np.arange(128)[None, :, None]
    k2 = np.arange(128)[None, None, :]
    angle = ((p2 * (k1 + 8 * k2)) % CH) * (2.0 * np.pi / CH)
    c, s = np.cos(angle), np.sin(angle)
    top = np.concatenate([c, -s], axis=2)
    low = np.concatenate([s, c], axis=2)
    return np.concatenate([top, low], axis=1).astype(jnp.bfloat16)


def iota(shape, dim):
    return lax.broadcasted_iota(jnp.int32, shape, dim)


def cos_turns(u):
    h = (u - jnp.round(u)) * math.pi
    q = h * h
    s = h * (1.0 + q * (-1.0 / 6 + q * (1.0 / 120 + q * (-1.0 / 5040 + q * (1.0 / 362880 - q * (1.0 / 39916800))))))
    return 1.0 - 2.0 * s * s


def nt_dot(a, b):
    return lax.dot_general(a, b, (((1,), (1,)), ((), ())), preferred_element_type=F32)


def rotated_taps(delay_s, proto_v, taps_a, taps_b, coef):
    taps = proto_v[...].astype(F32)
    for j in range(8):
        block = taps[:, 128 * j : 128 * j + 128]
        taps_a[pl.ds(j, TAPS, stride=8), :] = block
        taps_b[pl.ds((j + 1) % 8, TAPS, stride=8), :] = block
    lane = iota((128, 128), 1)

    def one(n, carry):
        d = delay_s[n]
        mixed = jnp.where(lane < 128 - d, taps_a[...], taps_b[...])
        coef[pl.ds(n, 128, stride=PAD), :] = pltpu.roll(mixed, d, 1)
        return carry

    lax.fori_loop(0, E_DEV, one, 0, unroll=8)


def delay_column(delay_s, column):
    row = iota((E_DEV, 128), 0)
    value = jnp.zeros((E_DEV, 128), jnp.int32)
    for n in range(E_DEV):
        value = jnp.where(row == n, delay_s[n], value)
    column[...] = value


def channel_rows(map_s, rows):
    row = iota((rows, 128), 0)
    which = ((row // 8) % 4) * 4 + row % 4
    value = jnp.zeros((rows, 128), jnp.int32)
    for s in range(16):
        value = jnp.where(which == s, map_s[s], value)
    return value.astype(F32)


def chosen_basis(map_s, basis):
    chan = channel_rows(map_s, 64) * (1.0 / CH)
    row = iota((64, 128), 0)
    swapped, second = row // 32, (row // 4) % 2
    zero = jnp.zeros((64, 128), F32)
    first_half = jnp.where(swapped == 0, jnp.where(second == 0, zero, 0.25), jnp.where(second == 0, -0.25, zero))
    last_half = jnp.where(swapped == 0, jnp.where(second == 0, -0.25, zero), jnp.where(second == 0, 0.5 + zero, -0.25))
    lane = iota((64, 128), 1)
    for j in range(8):
        turns = chan * (lane + 128 * j).astype(F32)
        basis[:, 128 * j : 128 * j + 128] = cos_turns(turns + first_half).astype(BF16)
        basis[:, CH + 128 * j : CH + 128 * j + 128] = cos_turns(turns + last_half).astype(BF16)


def filter_block(part, g, j, special, volt, coef, column, wave):
    rows = slice(16 * g, 16 * g + 16)

    def samples(b):
        start = b * CH + 128 * j
        if not isinstance(j, int):
            start = pl.multiple_of(start, 128)
        return volt[part, rows, pl.ds(start, 128)].astype(F32)

    sums = [None] * FRAMES
    if special:
        late = iota((16, 128), 1) < column[rows, :]
        following = samples(0)
    taps = {}
    for b in range(BLOCKS):
        if special:
            now = following
            following = samples(b + 1)
            value = jnp.where(late, following, now)
        else:
            value = samples(b)
        if b < TAPS:
            start = (b * 8 + j) * PAD + 16 * g
            if not isinstance(j, int):
                start = pl.multiple_of(start, 8)
            taps[b] = coef[pl.ds(start, 16), :]
        for f in range(FRAMES):
            t = b - f
            if 0 <= t < TAPS:
                term = taps[t] * value
                sums[f] = term if sums[f] is None else sums[f] + term
    column_start = part * CH + 128 * j
    if not isinstance(j, int):
        column_start = pl.multiple_of(column_start, 128)
    for f in range(FRAMES):
        wave[pl.ds(f * E_DEV + 16 * g, 16), pl.ds(column_start, 128)] = sums[f].astype(BF16)


def filter_chunk(part, g, volt, coef, column, wave):
    filter_block(part, g, 0, True, volt, coef, column, wave)

    def one(j, carry):
        filter_block(part, g, j, False, volt, coef, column, wave)
        return carry

    lax.fori_loop(1, 8, one, 0)


def chosen_spectra(delay_s, map_s, basis, wave, chosen):
    both = nt_dot(basis[...], wave[...])
    lane = iota((32, 128), 1) % E_DEV
    delay = jnp.zeros((32, 128), jnp.int32)
    for n in range(E_DEV):
        delay = jnp.where(lane == n, delay_s[n], delay)
    turns = channel_rows(map_s, 32) * delay.astype(F32) * (1.0 / CH)
    picked = both[:32] * cos_turns(turns) + both[32:] * cos_turns(turns - 0.25)
    picked = picked * (1.0 / math.sqrt(CH))
    for c in range(4):
        chosen[c] = picked[8 * c : 8 * c + 8].astype(BF16)


def butterflies(wave, halves):
    root = math.sqrt(0.5)

    def one(i, carry):
        rows = pl.ds(pl.multiple_of(16 * i, 16), 16)
        re = [wave[rows, 128 * j : 128 * j + 128].astype(F32) for j in range(8)]
        im = [wave[rows, CH + 128 * j : CH + 128 * j + 128].astype(F32) for j in range(8)]

        def four(ids):
            a, b, c, d = ids
            pr, pi, qr, qi = re[a] + re[c], im[a] + im[c], re[a] - re[c], im[a] - im[c]
            sr, si, tr, ti = re[b] + re[d], im[b] + im[d], re[b] - re[d], im[b] - im[d]
            return [(pr + sr, pi + si), (qr + ti, qi - tr), (pr - sr, pi - si), (qr - ti, qi + tr)]

        even, odd = four((0, 2, 4, 6)), four((1, 3, 5, 7))
        o1 = ((odd[1][0] + odd[1][1]) * root, (odd[1][1] - odd[1][0]) * root)
        o2 = (odd[2][1], -odd[2][0])
        o3 = ((odd[3][1] - odd[3][0]) * root, -(odd[3][0] + odd[3][1]) * root)
        turned = [odd[0], o1, o2, o3]
        for k in range(4):
            for sign in (0, 1):
                zr = even[k][0] - turned[k][0] if sign else even[k][0] + turned[k][0]
                zi = even[k][1] - turned[k][1] if sign else even[k][1] + turned[k][1]
                halves[k + 4 * sign, rows, 0:128] = zr.astype(BF16)
                halves[k + 4 * sign, rows, 128:256] = zi.astype(BF16)
        return carry

    lax.fori_loop(0, 8, one, 0)


def powers(halves, dft, power_k):
    def one(k, carry):
        spec = jnp.dot(halves[k], dft[k], preferred_element_type=F32)
        square = spec * spec
        total = square[:, 0:128] + square[:, 128:256]
        mean = total[0:32] + total[32:64] + total[64:96] + total[96:128]
        mean = mean * (1.0 / (FRAMES * CH))
        power_k[:, pl.ds(pl.multiple_of(128 * k, 128), 128)] = mean.astype(BF16)
        return carry

    lax.fori_loop(0, 8, one, 0)


def natural_order(power_k, power):
    source = iota((CH, 128), 0)
    target = source // 128 + 8 * (source % 128)

    def put(m, carry):
        select = jnp.where(target == iota((CH, 128), 1) + 128 * m, 1.0, 0.0).astype(BF16)
        block = jnp.dot(power_k[...], select, preferred_element_type=F32)
        power[:, pl.ds(pl.multiple_of(128 * m, 128), 128)] = block.astype(BF16)
        return carry

    lax.fori_loop(0, 8, put, 0)


def stack_weights(raw, rows_f32, weights):
    def one(i, carry):
        for k in range(8):
            piece = raw[k, :, pl.ds(pl.multiple_of(512 * i, 512), 512)].astype(F32)
            for m in range(4):
                start = 32 * m + 16 * (k % 2) + k // 2
                rows_f32[pl.ds(start, 4, stride=4), :] = piece[:, 128 * m : 128 * m + 128]
        for m in range(4):
            lanes = pl.ds(pl.multiple_of(512 * i + 128 * m, 128), 128)
            weights[:, lanes] = rows_f32[32 * m : 32 * m + 32, :].astype(BF16)
        return carry

    lax.fori_loop(0, 32, one, 0)


def regroup(arrived, first, out):
    lane = iota((8, 128), 1) // E_DEV
    blocks = [arrived[first + c].astype(F32) for c in range(4)]
    frames = []
    for f in range(FRAMES):
        value = None
        for c in range(4):
            shift = ((c - f) % 4) * E_DEV
            moved = pltpu.roll(blocks[c], shift, 1) if shift else blocks[c]
            value = moved if value is None else jnp.where(lane == c, moved, value)
        frames.append(value)
    out[...] = jnp.concatenate(frames, axis=0).astype(BF16)


def beams_out(total, rows, beams):
    row, col = iota((32, 128), 0), iota((32, 128), 1)
    same = jnp.where((row % 4 == (col // 4) % 4) & (col < 32), total[...], 0.0)
    folded = same + pltpu.roll(same, 124, 1) + pltpu.roll(same, 120, 1) + pltpu.roll(same, 116, 1)
    wide = folded.reshape(4, 8, 128)
    crossed = pltpu.roll(pltpu.roll(folded, 112, 1).reshape(4, 8, 128), 4, 1)
    real = iota((4, 8, 128), 1) < 4
    rows[...] = jnp.where(real, wide - crossed, wide + crossed).reshape(32, 128)
    ordered = jnp.concatenate([rows[pl.ds(k, 4, stride=8), :] for k in range(8)], axis=0)
    turned = ordered.T
    beams[0] = turned[0:4, 0:16]
    beams[1] = turned[0:4, 16:32]


def kernel(
    volt_h, delay_h, proto_h, map_h, raw_h, dft_h,
    power_h, beams,
    volt, delay_s, map_s, proto_v, taps_a, taps_b, coef, column, basis, wave, chosen, arrived,
    halves, dft, power_k, power, raw, rows_f32, weights, across_a, across_b, total, final,
    in_sem, volt_sem, out_sem, shot_send, shot_recv, hop_send, hop_recv,
):
    z, xl, y = lax.axis_index("z"), lax.axis_index("xl"), lax.axis_index("y")
    xh, core = lax.axis_index("xh"), lax.axis_index("core")
    chan = xh * 2 + core
    ahead_y = [lax.rem(y + r, RING) for r in range(RING)]
    ahead_z = [lax.rem(z + r, RING) for r in range(RING)]

    small = [
        pltpu.make_async_copy(delay_h, delay_s, in_sem.at[0]),
        pltpu.make_async_copy(map_h, map_s, in_sem.at[1]),
        pltpu.make_async_copy(proto_h, proto_v, in_sem.at[2]),
    ]
    for copy in small:
        copy.start()
    chunks = []
    for g in range(2):
        for part in range(2):
            rows = pl.ds(16 * g, 16)
            chunks.append(
                pltpu.make_async_copy(volt_h.at[part, rows, :], volt.at[part, rows, :], volt_sem.at[2 * g + part])
            )
    for copy in chunks:
        copy.start()
    later = [
        pltpu.make_async_copy(raw_h, raw, in_sem.at[3]),
        pltpu.make_async_copy(dft_h, dft, in_sem.at[4]),
    ]

    barrier = pltpu.get_barrier_semaphore()

    def hello(device):
        pl.semaphore_signal(barrier, inc=1, device_id=device, device_id_type=MESH)

    others = [lax.rem(chan + q, 4) for q in range(4)]
    for colour in range(2):
        for i in range(RING):
            for q in range(4):
                device = {"xl": colour, "xh": others[q] // 2, "core": lax.rem(others[q], 2)}
                device["z" if colour else "y"] = (ahead_z if colour else ahead_y)[i]
                if i == 0 and q == 0:
                    pl.when(xl != colour)(functools.partial(hello, device))
                else:
                    hello(device)
    for r in (1, 2, 6, 7):
        side_y = lax.rem(y + r * xl, RING)
        side_z = lax.rem(z + r * (1 - xl), RING)
        hello({"y": side_y, "z": side_z})

    for copy in small:
        copy.wait()
    delay_column(delay_s, column)
    rotated_taps(delay_s, proto_v, taps_a, taps_b, coef)
    chosen_basis(map_s, basis)
    for g in range(2):
        for part in range(2):
            chunks[2 * g + part].wait()
            if g == 1 and part == 1:
                for copy in later:
                    copy.start()
            filter_chunk(part, g, volt, coef, column, wave)
    chosen_spectra(delay_s, map_s, basis, wave, chosen)

    pl.semaphore_wait(barrier, 2 * RING * 4 - 1 + 4)

    line = xl * 4 + chan
    mine = xl * 32 + chan
    places = [lax.rem(line + q, LINE) for q in range(LINE)]
    for i in range(RING):
        r = ORDER[i]
        shot_y = lax.rem(y + r * (1 - xl), RING)
        shot_z = lax.rem(z + r * xl, RING)
        for q in (3, 5, 2, 6, 1, 7, 4, 0):
            if i == 0 and q == 0:
                continue
            place = places[q]
            pltpu.make_async_remote_copy(
                src_ref=chosen.at[lax.rem(place, 4)],
                dst_ref=arrived.at[mine + 4 * i],
                send_sem=shot_send,
                recv_sem=shot_recv.at[xl * RING + i],
                device_id={
                    "xl": place // 4, "xh": lax.rem(place // 2, 2), "core": lax.rem(place, 2),
                    "y": shot_y, "z": shot_z,
                },
                device_id_type=MESH,
            ).start()
    arrived[mine] = chosen[chan]

    later[0].wait()
    stack_weights(raw, rows_f32, weights)
    butterflies(wave, halves)

    across = (across_a, across_b)
    aside = ("z", "y")
    ahead = (ahead_z, ahead_y)

    def shot(colour, i, count):
        return pltpu.make_async_remote_copy(
            src_ref=arrived.at[pl.ds(0, count)],
            dst_ref=arrived.at[pl.ds(colour * 32 + 4 * i, count)],
            send_sem=shot_send,
            recv_sem=shot_recv.at[colour * RING + i],
            device_id={"y": ahead_y[1]},
            device_id_type=MESH,
        )

    def ready(colour, i):
        if i:
            shot(colour, i, 4).wait_recv()
        else:
            pl.when(xl == colour)(lambda: shot(colour, i, 3).wait_recv())
            pl.when(xl != colour)(lambda: shot(colour, i, 4).wait_recv())
        regroup(arrived, colour * 32 + 4 * i, across[colour].at[0, i])

    def hop(colour, way, kind, i):
        sign = -1 if way else 1
        held = (0, 0, 2, 2)[kind] * sign % RING
        step = (1, 2, 1, 2)[kind] * sign % RING
        return pltpu.make_async_remote_copy(
            src_ref=across[colour].at[held, i],
            dst_ref=across[colour].at[(held + step) % RING, i],
            send_sem=hop_send.at[colour, way, kind],
            recv_sem=hop_recv.at[colour, way, kind, i],
            device_id={aside[colour]: ahead[colour][step]},
            device_id_type=MESH,
        )

    total[...] = jnp.zeros_like(total)

    def add(pieces):
        data, weight = [], []
        for colour, held, i in pieces:
            zz = ahead_z[(RING - (held if colour == 0 else ORDER[i])) % RING]
            yy = ahead_y[(RING - (ORDER[i] if colour == 0 else held)) % RING]
            block = (zz * 2 + colour) * RING + yy
            data.append(across[colour][held, i])
            weight.append(weights[:, pl.ds(pl.multiple_of(block * 128, 128), 128)])
        total[:, 0:32] += nt_dot(jnp.concatenate(data, axis=1), jnp.concatenate(weight, axis=1))

    for i in range(RING):
        for colour in range(2):
            ready(colour, i)
            for way in range(2):
                hop(colour, way, 1, i).start()
                hop(colour, way, 0, i).start()

    later[1].wait()
    powers(halves, dft, power_k)
    pieces = []
    for i in range(RING):
        for colour in range(2):
            for way in range(2):
                hop(colour, way, 1, i).wait_recv()
                if i % 2 == way:
                    hop(colour, way, 3, i).start()
                hop(colour, way, 2, i).start()
    natural_order(power_k, power)
    power_out = pltpu.make_async_copy(power, power_h, out_sem)
    power_out.start()
    add([(colour, 0, i) for colour in range(2) for i in range(RING)])
    for i in range(RING):
        for colour in range(2):
            for way in range(2):
                hop(colour, way, 0, i).wait_recv()
    for held in (1, 2, 6, 7):
        add([(colour, held, i) for colour in range(2) for i in range(RING)])
    pltpu.make_async_remote_copy(
        src_ref=arrived.at[pl.ds(0, 63)],
        dst_ref=arrived.at[pl.ds(0, 63)],
        send_sem=shot_send,
        recv_sem=shot_recv.at[0],
        device_id={"y": ahead_y[1]},
        device_id_type=MESH,
    ).wait_send()
    for pair in range(4):
        pieces = []
        for i in (2 * pair, 2 * pair + 1):
            for colour in range(2):
                for way in range(2):
                    hop(colour, way, 2, i).wait_recv()
                    pieces.append((colour, 5 if way else 3, i))
                    if i % 2 == way:
                        hop(colour, way, 3, i).wait_recv()
                        pieces.append((colour, 4, i))
        add(pieces)
    beams_out(total, final, beams)

    for colour in range(2):
        for way in range(2):
            for kind in range(4):
                count = 4 if kind == 3 else 8
                pltpu.make_async_remote_copy(
                    src_ref=across[colour].at[0, pl.ds(0, count)],
                    dst_ref=across[colour].at[0, pl.ds(0, count)],
                    send_sem=hop_send.at[colour, way, kind],
                    recv_sem=hop_recv.at[colour, way, kind, 0],
                    device_id={"y": ahead_y[1]},
                    device_id_type=MESH,
                ).wait_send()
    power_out.wait()


def on_device(voltages, delays, prototype, subband_map, beam_weights):
    raw = beam_weights.reshape(8, 4, 16384)
    dft = jnp.asarray(dft_blocks())
    any_spec = pl.BlockSpec(memory_space=pl.ANY)
    dma = pltpu.SemaphoreType.DMA
    power, beams = pl.pallas_call(
        kernel,
        out_shape=(
            jax.ShapeDtypeStruct((E_DEV, CH), BF16),
            jax.ShapeDtypeStruct((2, 4, 16), F32),
        ),
        in_specs=[any_spec] * 6,
        out_specs=(any_spec, pl.BlockSpec(memory_space=pltpu.VMEM)),
        scratch_shapes=[
            pltpu.VMEM((2, E_DEV, SAMP), BF16),
            pltpu.SMEM((E_DEV,), jnp.int32),
            pltpu.SMEM((16,), jnp.int32),
            pltpu.VMEM((TAPS, CH), BF16),
            pltpu.VMEM((128, 128), F32),
            pltpu.VMEM((128, 128), F32),
            pltpu.VMEM((128 * PAD, 128), F32),
            pltpu.VMEM((E_DEV, 128), jnp.int32),
            pltpu.VMEM((64, 2 * CH), BF16),
            pltpu.VMEM((128, 2 * CH), BF16),
            pltpu.VMEM((4, 8, 128), BF16),
            pltpu.VMEM((64, 8, 128), BF16),
            pltpu.VMEM((8, 128, 256), BF16),
            pltpu.VMEM((8, 256, 256), BF16),
            pltpu.VMEM((E_DEV, CH), BF16),
            pltpu.VMEM((E_DEV, CH), BF16),
            pltpu.VMEM((8, 4, 16384), BF16),
            pltpu.VMEM((128, 128), F32),
            pltpu.VMEM((32, 16384), BF16),
            pltpu.VMEM((RING, RING, 32, 128), BF16),
            pltpu.VMEM((RING, RING, 32, 128), BF16),
            pltpu.VMEM((32, 128), F32),
            pltpu.VMEM((32, 128), F32),
            dma((5,)),
            dma((4,)),
            dma,
            dma,
            dma((2 * RING,)),
            dma((2, 2, 4)),
            dma((2, 2, 4, RING)),
        ],
        compiler_params=pltpu.CompilerParams(collective_id=0, has_side_effects=True),
        name="channelize_and_beamform",
    )(voltages, delays, prototype, subband_map, raw, dft)
    beams = jnp.transpose(beams, (0, 2, 1))
    return power, beams


def solution(mesh):
    finer = Mesh(mesh.devices.reshape(8, 2, 8, 2, 2), ("z", "xl", "y", "xh", "core"))
    elem, chan = ("z", "xl", "y"), ("xh", "core")
    placed = (P(None, elem + chan, None), P(elem + chan), P(), P(), P(elem, None, chan, None))
    return jax.shard_map(
        on_device,
        mesh=finer,
        in_specs=placed,
        out_specs=(P(elem + chan, None), P(None, chan, elem)),
        check_vma=False,
    )
```

```python
import functools
import math

import numpy as np
import jax
import jax.numpy as jnp
from jax import lax
from jax.experimental import pallas as pl
from jax.experimental.pallas import tpu as pltpu
from jax.sharding import Mesh
from jax.sharding import PartitionSpec as P

MESH = pl.DeviceIdType.MESH
CH, TAPS, FRAMES, E_DEV = 1024, 16, 4, 32
BLOCKS = FRAMES + TAPS - 1
SAMP = 19584
RING = 8
LINE = 8
PAD = 40
ORDER = (0, 1, 7, 2, 6, 3, 5, 4)
F32, BF16 = jnp.float32, jnp.bfloat16


def dft_blocks():
    k1 = np.arange(8)[:, None, None]
    p2 = np.arange(128)[None, :, None]
    k2 = np.arange(128)[None, None, :]
    angle = ((p2 * (k1 + 8 * k2)) % CH) * (2.0 * np.pi / CH)
    c, s = np.cos(angle), np.sin(angle)
    top = np.concatenate([c, -s], axis=2)
    low = np.concatenate([s, c], axis=2)
    return np.concatenate([top, low], axis=1).astype(jnp.bfloat16)


def iota(shape, dim):
    return lax.broadcasted_iota(jnp.int32, shape, dim)


def cos_turns(u):
    h = (u - jnp.round(u)) * math.pi
    q = h * h
    s = h * (1.0 + q * (-1.0 / 6 + q * (1.0 / 120 + q * (-1.0 / 5040 + q * (1.0 / 362880 - q * (1.0 / 39916800))))))
    return 1.0 - 2.0 * s * s


def nt_dot(a, b):
    return lax.dot_general(a, b, (((1,), (1,)), ((), ())), preferred_element_type=F32)


def rotated_taps(delay_s, proto_v, taps_a, taps_b, coef):
    taps = proto_v[...].astype(F32)
    for j in range(8):
        block = taps[:, 128 * j : 128 * j + 128]
        taps_a[pl.ds(j, TAPS, stride=8), :] = block
        taps_b[pl.ds((j + 1) % 8, TAPS, stride=8), :] = block
    lane = iota((128, 128), 1)

    def one(n, carry):
        d = delay_s[n]
        mixed = jnp.where(lane < 128 - d, taps_a[...], taps_b[...])
        coef[pl.ds(n, 128, stride=PAD), :] = pltpu.roll(mixed, d, 1)
        return carry

    lax.fori_loop(0, E_DEV, one, 0, unroll=16)


def delay_column(delay_s, column):
    row = iota((E_DEV, 128), 0)
    value = jnp.zeros((E_DEV, 128), jnp.int32)
    for n in range(E_DEV):
        value = jnp.where(row == n, delay_s[n], value)
    column[...] = value


def channel_rows(map_s, rows):
    row = iota((rows, 128), 0)
    which = ((row // 8) % 4) * 4 + row % 4
    value = jnp.zeros((rows, 128), jnp.int32)
    for s in range(16):
        value = jnp.where(which == s, map_s[s], value)
    return value.astype(F32)


def chosen_basis(map_s, basis):
    chan = channel_rows(map_s, 32) * (1.0 / CH)
    second = (iota((32, 128), 0) // 4) % 2
    of_real = jnp.where(second == 0, 0.0, 0.25)
    of_imag = jnp.where(second == 0, -0.25, 0.0)
    lane = iota((32, 128), 1)
    for j in range(8):
        turns = chan * (lane + 128 * j).astype(F32)
        a = cos_turns(turns + of_real).astype(BF16)
        b = cos_turns(turns + of_imag).astype(BF16)
        left, right = slice(128 * j, 128 * j + 128), slice(CH + 128 * j, CH + 128 * j + 128)
        basis[0:32, left] = a
        basis[0:32, right] = b
        basis[32:64, left] = b
        basis[32:64, right] = -a


def filter_block(part, g, j, special, volt, coef, column, wave):
    rows = slice(16 * g, 16 * g + 16)

    def samples(b):
        start = b * CH + 128 * j
        if not isinstance(j, int):
            start = pl.multiple_of(start, 128)
        return volt[part, rows, pl.ds(start, 128)].astype(F32)

    sums = [None] * FRAMES
    if special:
        late = iota((16, 128), 1) < column[rows, :]
        following = samples(0)
    taps = {}
    for b in range(BLOCKS):
        if special:
            now = following
            following = samples(b + 1)
            value = jnp.where(late, following, now)
        else:
            value = samples(b)
        if b < TAPS:
            start = (b * 8 + j) * PAD + 16 * g
            if not isinstance(j, int):
                start = pl.multiple_of(start, 8)
            taps[b] = coef[pl.ds(start, 16), :]
        for f in range(FRAMES):
            t = b - f
            if 0 <= t < TAPS:
                term = taps[t] * value
                sums[f] = term if sums[f] is None else sums[f] + term
    column_start = part * CH + 128 * j
    if not isinstance(j, int):
        column_start = pl.multiple_of(column_start, 128)
    for f in range(FRAMES):
        wave[pl.ds(f * E_DEV + 16 * g, 16), pl.ds(column_start, 128)] = sums[f].astype(BF16)


def filter_chunk(part, g, volt, coef, column, wave):
    filter_block(part, g, 0, True, volt, coef, column, wave)

    def one(j, carry):
        filter_block(part, g, j, False, volt, coef, column, wave)
        return carry

    lax.fori_loop(1, 8, one, 0)


def chosen_spectra(delay_s, map_s, basis, wave, chosen):
    both = nt_dot(basis[...], wave[...])
    lane = iota((32, 128), 1) % E_DEV
    delay = jnp.zeros((32, 128), jnp.int32)
    for n in range(E_DEV):
        delay = jnp.where(lane == n, delay_s[n], delay)
    turns = channel_rows(map_s, 32) * delay.astype(F32) * (1.0 / CH)
    picked = both[:32] * cos_turns(turns) + both[32:] * cos_turns(turns - 0.25)
    picked = picked * (1.0 / math.sqrt(CH))
    for c in range(4):
        chosen[c] = picked[8 * c : 8 * c + 8].astype(BF16)


def butterflies(wave, halves):
    root = math.sqrt(0.5)

    def one(i, carry):
        rows = pl.ds(pl.multiple_of(16 * i, 16), 16)
        re = [wave[rows, 128 * j : 128 * j + 128].astype(F32) for j in range(8)]
        im = [wave[rows, CH + 128 * j : CH + 128 * j + 128].astype(F32) for j in range(8)]

        def four(ids):
            a, b, c, d = ids
            pr, pi, qr, qi = re[a] + re[c], im[a] + im[c], re[a] - re[c], im[a] - im[c]
            sr, si, tr, ti = re[b] + re[d], im[b] + im[d], re[b] - re[d], im[b] - im[d]
            return [(pr + sr, pi + si), (qr + ti, qi - tr), (pr - sr, pi - si), (qr - ti, qi + tr)]

        even, odd = four((0, 2, 4, 6)), four((1, 3, 5, 7))
        o1 = ((odd[1][0] + odd[1][1]) * root, (odd[1][1] - odd[1][0]) * root)
        o2 = (odd[2][1], -odd[2][0])
        o3 = ((odd[3][1] - odd[3][0]) * root, -(odd[3][0] + odd[3][1]) * root)
        turned = [odd[0], o1, o2, o3]
        for k in range(4):
            for sign in (0, 1):
                zr = even[k][0] - turned[k][0] if sign else even[k][0] + turned[k][0]
                zi = even[k][1] - turned[k][1] if sign else even[k][1] + turned[k][1]
                halves[k + 4 * sign, rows, 0:128] = zr.astype(BF16)
                halves[k + 4 * sign, rows, 128:256] = zi.astype(BF16)
        return carry

    lax.fori_loop(0, 8, one, 0)


def powers(halves, dft, power_k):
    def one(k, carry):
        spec = jnp.dot(halves[k], dft[k], preferred_element_type=F32)
        square = spec * spec
        total = square[:, 0:128] + square[:, 128:256]
        mean = total[0:32] + total[32:64] + total[64:96] + total[96:128]
        mean = mean * (1.0 / (FRAMES * CH))
        lanes = pl.ds(pl.multiple_of(128 * k, 128), 128)
        for m in range(8):
            moved = pltpu.roll(mean, 128 - 16 * m, 1) if m else mean
            power_k[32 * m : 32 * m + 32, lanes] = moved.astype(BF16)
        return carry

    lax.fori_loop(0, 8, one, 0, unroll=2)


def natural_order(power_k, power):
    source, lane = iota((CH, 128), 0), iota((CH, 128), 1)
    select = jnp.where(lane == source // 128 + 8 * (source % 128), 1.0, 0.0).astype(BF16)
    ordered = jnp.dot(power_k[...], select, preferred_element_type=F32)
    for m in range(8):
        power[:, 128 * m : 128 * m + 128] = ordered[32 * m : 32 * m + 32].astype(BF16)


def stack_weights(raw, rows_f32, weights):
    def one(i, carry):
        for k in range(8):
            piece = raw[k, :, pl.ds(pl.multiple_of(512 * i, 512), 512)].astype(F32)
            for m in range(4):
                start = 32 * m + 16 * (k % 2) + k // 2
                rows_f32[pl.ds(start, 4, stride=4), :] = piece[:, 128 * m : 128 * m + 128]
        for m in range(4):
            lanes = pl.ds(pl.multiple_of(512 * i + 128 * m, 128), 128)
            weights[:, lanes] = rows_f32[32 * m : 32 * m + 32, :].astype(BF16)
        return carry

    lax.fori_loop(0, 32, one, 0)


def regroup(arrived, first, out):
    lane = iota((8, 128), 1) // E_DEV
    blocks = [arrived[first + c].astype(F32) for c in range(4)]
    frames = []
    for f in range(FRAMES):
        value = None
        for c in range(4):
            shift = ((c - f) % 4) * E_DEV
            moved = pltpu.roll(blocks[c], shift, 1) if shift else blocks[c]
            value = moved if value is None else jnp.where(lane == c, moved, value)
        frames.append(value)
    out[...] = jnp.concatenate(frames, axis=0).astype(BF16)


def beams_out(total, rows, beams):
    row, col = iota((32, 128), 0), iota((32, 128), 1)
    same = jnp.where((row % 4 == (col // 4) % 4) & (col < 32), total[...], 0.0)
    folded = same + pltpu.roll(same, 124, 1) + pltpu.roll(same, 120, 1) + pltpu.roll(same, 116, 1)
    wide = folded.reshape(4, 8, 128)
    crossed = pltpu.roll(pltpu.roll(folded, 112, 1).reshape(4, 8, 128), 4, 1)
    real = iota((4, 8, 128), 1) < 4
    rows[...] = jnp.where(real, wide - crossed, wide + crossed).reshape(32, 128)
    ordered = jnp.concatenate([rows[pl.ds(k, 4, stride=8), :] for k in range(8)], axis=0)
    turned = ordered.T
    beams[0] = turned[0:4, 0:16]
    beams[1] = turned[0:4, 16:32]


def kernel(
    volt_h, delay_h, proto_h, map_h, raw_h, dft_h,
    power, beams,
    volt, delay_s, map_s, proto_v, taps_a, taps_b, coef, column, basis, wave, chosen, arrived,
    halves, dft, power_k, raw, rows_f32, weights, across_a, across_b, total, final,
    in_sem, volt_sem, shot_send, shot_recv, hop_send, hop_recv,
):
    z, xl, y = lax.axis_index("z"), lax.axis_index("xl"), lax.axis_index("y")
    xh, core = lax.axis_index("xh"), lax.axis_index("core")
    chan = xh * 2 + core
    ahead_y = [lax.rem(y + r, RING) for r in range(RING)]
    ahead_z = [lax.rem(z + r, RING) for r in range(RING)]

    small = [
        pltpu.make_async_copy(delay_h, delay_s, in_sem.at[0]),
        pltpu.make_async_copy(map_h, map_s, in_sem.at[1]),
        pltpu.make_async_copy(proto_h, proto_v, in_sem.at[2]),
    ]
    for copy in small:
        copy.start()
    chunks = []
    for g in range(2):
        for part in range(2):
            rows = pl.ds(16 * g, 16)
            chunks.append(
                pltpu.make_async_copy(volt_h.at[part, rows, :], volt.at[part, rows, :], volt_sem.at[2 * g + part])
            )
    for copy in chunks:
        copy.start()
    later = [
        pltpu.make_async_copy(raw_h, raw, in_sem.at[3]),
        pltpu.make_async_copy(dft_h, dft, in_sem.at[4]),
    ]

    barrier = pltpu.get_barrier_semaphore()

    def hello(device):
        pl.semaphore_signal(barrier, inc=1, device_id=device, device_id_type=MESH)

    others = [lax.rem(chan + q, 4) for q in range(4)]
    for colour in range(2):
        for i in range(RING):
            for q in range(4):
                device = {"xl": colour, "xh": others[q] // 2, "core": lax.rem(others[q], 2)}
                device["z" if colour else "y"] = (ahead_z if colour else ahead_y)[i]
                if i == 0 and q == 0:
                    pl.when(xl != colour)(functools.partial(hello, device))
                else:
                    hello(device)
    for r in (1, 2, 6, 7):
        side_y = lax.rem(y + r * xl, RING)
        side_z = lax.rem(z + r * (1 - xl), RING)
        hello({"y": side_y, "z": side_z})

    for copy in small:
        copy.wait()
    delay_column(delay_s, column)
    rotated_taps(delay_s, proto_v, taps_a, taps_b, coef)
    chosen_basis(map_s, basis)
    for g in range(2):
        for part in range(2):
            chunks[2 * g + part].wait()
            if g == 1 and part == 1:
                for copy in later:
                    copy.start()
            filter_chunk(part, g, volt, coef, column, wave)
    chosen_spectra(delay_s, map_s, basis, wave, chosen)

    pl.semaphore_wait(barrier, 2 * RING * 4 - 1 + 4)

    line = xl * 4 + chan
    mine = xl * 32 + chan
    places = [lax.rem(line + q, LINE) for q in range(LINE)]
    for i in range(RING):
        r = ORDER[i]
        shot_y = lax.rem(y + r * (1 - xl), RING)
        shot_z = lax.rem(z + r * xl, RING)
        for q in (3, 5, 2, 6, 1, 7, 4, 0):
            if i == 0 and q == 0:
                continue
            place = places[q]
            pltpu.make_async_remote_copy(
                src_ref=chosen.at[lax.rem(place, 4)],
                dst_ref=arrived.at[mine + 4 * i],
                send_sem=shot_send,
                recv_sem=shot_recv.at[xl * RING + i],
                device_id={
                    "xl": place // 4, "xh": lax.rem(place // 2, 2), "core": lax.rem(place, 2),
                    "y": shot_y, "z": shot_z,
                },
                device_id_type=MESH,
            ).start()
    arrived[mine] = chosen[chan]

    later[0].wait()
    stack_weights(raw, rows_f32, weights)
    butterflies(wave, halves)
    later[1].wait()
    powers(halves, dft, power_k)

    across = (across_a, across_b)
    aside = ("z", "y")
    ahead = (ahead_z, ahead_y)

    def shot(colour, i, count):
        return pltpu.make_async_remote_copy(
            src_ref=arrived.at[pl.ds(0, count)],
            dst_ref=arrived.at[pl.ds(colour * 32 + 4 * i, count)],
            send_sem=shot_send,
            recv_sem=shot_recv.at[colour * RING + i],
            device_id={"y": ahead_y[1]},
            device_id_type=MESH,
        )

    def ready(colour, i):
        if i:
            shot(colour, i, 4).wait_recv()
        else:
            pl.when(xl == colour)(lambda: shot(colour, i, 3).wait_recv())
            pl.when(xl != colour)(lambda: shot(colour, i, 4).wait_recv())
        regroup(arrived, colour * 32 + 4 * i, across[colour].at[0, i])

    def hop(colour, way, kind, i):
        sign = -1 if way else 1
        held = (0, 0, 2, 2)[kind] * sign % RING
        step = (1, 2, 1, 2)[kind] * sign % RING
        return pltpu.make_async_remote_copy(
            src_ref=across[colour].at[held, i],
            dst_ref=across[colour].at[(held + step) % RING, i],
            send_sem=hop_send.at[colour, way, kind],
            recv_sem=hop_recv.at[colour, way, kind, i],
            device_id={aside[colour]: ahead[colour][step]},
            device_id_type=MESH,
        )

    total[...] = jnp.zeros_like(total)

    def add(pieces):
        data, weight = [], []
        for colour, held, i in pieces:
            zz = ahead_z[(RING - (held if colour == 0 else ORDER[i])) % RING]
            yy = ahead_y[(RING - (ORDER[i] if colour == 0 else held)) % RING]
            block = (zz * 2 + colour) * RING + yy
            data.append(across[colour][held, i])
            weight.append(weights[:, pl.ds(pl.multiple_of(block * 128, 128), 128)])
        total[:, 0:32] += nt_dot(jnp.concatenate(data, axis=1), jnp.concatenate(weight, axis=1))

    for i in range(RING):
        for colour in range(2):
            ready(colour, i)
            for way in range(2):
                hop(colour, way, 1, i).start()
                hop(colour, way, 0, i).start()

    for i in range(RING):
        for colour in range(2):
            for way in range(2):
                hop(colour, way, 1, i).wait_recv()
                if i % 2 == way:
                    hop(colour, way, 3, i).start()
                hop(colour, way, 2, i).start()
    natural_order(power_k, power)
    add([(colour, 0, i) for colour in range(2) for i in range(RING)])
    for i in range(RING):
        for colour in range(2):
            for way in range(2):
                hop(colour, way, 0, i).wait_recv()
    for held in (1, 2, 6, 7):
        add([(colour, held, i) for colour in range(2) for i in range(RING)])
    pltpu.make_async_remote_copy(
        src_ref=arrived.at[pl.ds(0, 63)],
        dst_ref=arrived.at[pl.ds(0, 63)],
        send_sem=shot_send,
        recv_sem=shot_recv.at[0],
        device_id={"y": ahead_y[1]},
        device_id_type=MESH,
    ).wait_send()
    for pair in range(4):
        pieces = []
        for i in (2 * pair, 2 * pair + 1):
            for colour in range(2):
                for way in range(2):
                    hop(colour, way, 2, i).wait_recv()
                    pieces.append((colour, 5 if way else 3, i))
                    if i % 2 == way:
                        hop(colour, way, 3, i).wait_recv()
                        pieces.append((colour, 4, i))
        add(pieces)
    beams_out(total, final, beams)

    for colour in range(2):
        for way in range(2):
            for kind in range(4):
                count = 4 if kind == 3 else 8
                pltpu.make_async_remote_copy(
                    src_ref=across[colour].at[0, pl.ds(0, count)],
                    dst_ref=across[colour].at[0, pl.ds(0, count)],
                    send_sem=hop_send.at[colour, way, kind],
                    recv_sem=hop_recv.at[colour, way, kind, 0],
                    device_id={"y": ahead_y[1]},
                    device_id_type=MESH,
                ).wait_send()


def on_device(voltages, delays, prototype, subband_map, beam_weights):
    arrays = (voltages, delays, prototype, subband_map, beam_weights.reshape(8, 4, 16384), jnp.asarray(dft_blocks()))
    arrays = [pltpu.with_memory_space_constraint(array, pltpu.HBM) for array in arrays]
    any_spec = pl.BlockSpec(memory_space=pl.ANY)
    dma = pltpu.SemaphoreType.DMA
    power, beams = pl.pallas_call(
        kernel,
        out_shape=(
            jax.ShapeDtypeStruct((E_DEV, CH), BF16),
            jax.ShapeDtypeStruct((2, 4, 16), F32),
        ),
        in_specs=[any_spec] * 6,
        out_specs=(pl.BlockSpec(memory_space=pltpu.VMEM), pl.BlockSpec(memory_space=pltpu.VMEM)),
        scratch_shapes=[
            pltpu.VMEM((2, E_DEV, SAMP), BF16),
            pltpu.SMEM((E_DEV,), jnp.int32),
            pltpu.SMEM((16,), jnp.int32),
            pltpu.VMEM((TAPS, CH), BF16),
            pltpu.VMEM((128, 128), F32),
            pltpu.VMEM((128, 128), F32),
            pltpu.VMEM((128 * PAD, 128), F32),
            pltpu.VMEM((E_DEV, 128), jnp.int32),
            pltpu.VMEM((64, 2 * CH), BF16),
            pltpu.VMEM((128, 2 * CH), BF16),
            pltpu.VMEM((4, 8, 128), BF16),
            pltpu.VMEM((64, 8, 128), BF16),
            pltpu.VMEM((8, 128, 256), BF16),
            pltpu.VMEM((8, 256, 256), BF16),
            pltpu.VMEM((8 * E_DEV, CH), BF16),
            pltpu.VMEM((8, 4, 16384), BF16),
            pltpu.VMEM((128, 128), F32),
            pltpu.VMEM((32, 16384), BF16),
            pltpu.VMEM((RING, RING, 32, 128), BF16),
            pltpu.VMEM((RING, RING, 32, 128), BF16),
            pltpu.VMEM((32, 128), F32),
            pltpu.VMEM((32, 128), F32),
            dma((5,)),
            dma((4,)),
            dma,
            dma((2 * RING,)),
            dma((2, 2, 4)),
            dma((2, 2, 4, RING)),
        ],
        compiler_params=pltpu.CompilerParams(collective_id=0, has_side_effects=True, vmem_limit_bytes=48_000_000),
        name="channelize_and_beamform",
    )(*arrays)
    beams = jnp.transpose(beams, (0, 2, 1))
    return power, beams


def solution(mesh):
    finer = Mesh(mesh.devices.reshape(8, 2, 8, 2, 2), ("z", "xl", "y", "xh", "core"))
    elem, chan = ("z", "xl", "y"), ("xh", "core")
    placed = (P(None, elem + chan, None), P(elem + chan), P(), P(), P(elem, None, chan, None))
    return jax.shard_map(
        on_device,
        mesh=finer,
        in_specs=placed,
        out_specs=(P(elem + chan, None), P(None, chan, elem)),
        check_vma=False,
    )
```

```python
import functools
import math

import numpy as np
import jax
import jax.numpy as jnp
from jax import lax
from jax.experimental import pallas as pl
from jax.experimental.pallas import tpu as pltpu
from jax.sharding import Mesh
from jax.sharding import PartitionSpec as P

MESH = pl.DeviceIdType.MESH
CH, TAPS, FRAMES, E_DEV = 1024, 16, 4, 32
BLOCKS = FRAMES + TAPS - 1
SAMP = 19584
RING = 8
LINE = 8
PAD = 36
ORDER = (0, 1, 7, 2, 6, 3, 5, 4)
F32, BF16 = jnp.float32, jnp.bfloat16


def dft_blocks():
    k1 = np.arange(8)[:, None, None]
    p2 = np.arange(128)[None, :, None]
    k2 = np.arange(128)[None, None, :]
    angle = ((p2 * (k1 + 8 * k2)) % CH) * (2.0 * np.pi / CH)
    c, s = np.cos(angle), np.sin(angle)
    top = np.concatenate([c, -s], axis=2)
    low = np.concatenate([s, c], axis=2)
    return np.concatenate([top, low], axis=1).astype(jnp.bfloat16)


def iota(shape, dim):
    return lax.broadcasted_iota(jnp.int32, shape, dim)


def cos_turns(u):
    h = (u - jnp.round(u)) * math.pi
    q = h * h
    s = h * (1.0 + q * (-1.0 / 6 + q * (1.0 / 120 + q * (-1.0 / 5040 + q * (1.0 / 362880 - q * (1.0 / 39916800))))))
    return 1.0 - 2.0 * s * s


def nt_dot(a, b):
    return lax.dot_general(a, b, (((1,), (1,)), ((), ())), preferred_element_type=F32)


def rotated_taps(delay_s, proto_v, taps_a, taps_b, coef):
    taps = proto_v[...].astype(F32)
    for j in range(8):
        block = taps[:, 128 * j : 128 * j + 128]
        taps_a[pl.ds(j, TAPS, stride=8), :] = block
        taps_b[pl.ds((j + 1) % 8, TAPS, stride=8), :] = block
    lane = iota((128, 128), 1)

    def one(n, carry):
        d = delay_s[n]
        mixed = jnp.where(lane < 128 - d, taps_a[...], taps_b[...])
        coef[pl.ds(n, 128, stride=PAD), :] = pltpu.roll(mixed, d, 1)
        return carry

    lax.fori_loop(0, E_DEV, one, 0, unroll=16)


def delay_column(delay_s, column):
    row = iota((E_DEV, 128), 0)
    value = jnp.zeros((E_DEV, 128), jnp.int32)
    for n in range(E_DEV):
        value = jnp.where(row == n, delay_s[n], value)
    column[...] = value


def channel_rows(map_s, rows):
    row = iota((rows, 128), 0)
    which = ((row // 8) % 4) * 4 + row % 4
    value = jnp.zeros((rows, 128), jnp.int32)
    for s in range(16):
        value = jnp.where(which == s, map_s[s], value)
    return value.astype(F32)


def chosen_basis(map_s, basis):
    chan = channel_rows(map_s, 32) * (1.0 / CH)
    second = (iota((32, 128), 0) // 4) % 2
    of_real = jnp.where(second == 0, 0.0, 0.25)
    of_imag = jnp.where(second == 0, -0.25, 0.0)
    lane = iota((32, 128), 1)
    for j in range(8):
        turns = chan * (lane + 128 * j).astype(F32)
        a = cos_turns(turns + of_real).astype(BF16)
        b = cos_turns(turns + of_imag).astype(BF16)
        left, right = slice(128 * j, 128 * j + 128), slice(CH + 128 * j, CH + 128 * j + 128)
        basis[0:32, left] = a
        basis[0:32, right] = b
        basis[32:64, left] = b
        basis[32:64, right] = -a


def filter_block(part, g, j, special, volt, coef, column, wave):
    rows = slice(16 * g, 16 * g + 16)

    def samples(b):
        start = b * CH + 128 * j
        if not isinstance(j, int):
            start = pl.multiple_of(start, 128)
        return volt[part, rows, pl.ds(start, 128)].astype(F32)

    sums = [None] * FRAMES
    if special:
        late = iota((16, 128), 1) < column[rows, :]
        following = samples(0)
    taps = {}
    for b in range(BLOCKS):
        if special:
            now = following
            following = samples(b + 1)
            value = jnp.where(late, following, now)
        else:
            value = samples(b)
        if b < TAPS:
            start = (b * 8 + j) * PAD + 16 * g
            if not isinstance(j, int):
                start = pl.multiple_of(start, 4)
            taps[b] = coef[pl.ds(start, 16), :]
        for f in range(FRAMES):
            t = b - f
            if 0 <= t < TAPS:
                term = taps[t] * value
                sums[f] = term if sums[f] is None else sums[f] + term
    column_start = part * CH + 128 * j
    if not isinstance(j, int):
        column_start = pl.multiple_of(column_start, 128)
    for f in range(FRAMES):
        wave[pl.ds(f * E_DEV + 16 * g, 16), pl.ds(column_start, 128)] = sums[f].astype(BF16)


def filter_chunk(part, g, volt, coef, column, wave):
    filter_block(part, g, 0, True, volt, coef, column, wave)

    def one(j, carry):
        filter_block(part, g, j, False, volt, coef, column, wave)
        return carry

    lax.fori_loop(1, 8, one, 0)


def chosen_spectra(delay_s, map_s, basis, wave, chosen):
    both = nt_dot(basis[...], wave[...])
    lane = iota((32, 128), 1) % E_DEV
    delay = jnp.zeros((32, 128), jnp.int32)
    for n in range(E_DEV):
        delay = jnp.where(lane == n, delay_s[n], delay)
    turns = channel_rows(map_s, 32) * delay.astype(F32) * (1.0 / CH)
    picked = both[:32] * cos_turns(turns) + both[32:] * cos_turns(turns - 0.25)
    picked = picked * (1.0 / math.sqrt(CH))
    for c in range(4):
        chosen[c] = picked[8 * c : 8 * c + 8].astype(BF16)


def butterflies(wave, halves):
    root = math.sqrt(0.5)

    def one(i, carry):
        rows = pl.ds(pl.multiple_of(16 * i, 16), 16)
        re = [wave[rows, 128 * j : 128 * j + 128].astype(F32) for j in range(8)]
        im = [wave[rows, CH + 128 * j : CH + 128 * j + 128].astype(F32) for j in range(8)]

        def four(ids):
            a, b, c, d = ids
            pr, pi, qr, qi = re[a] + re[c], im[a] + im[c], re[a] - re[c], im[a] - im[c]
            sr, si, tr, ti = re[b] + re[d], im[b] + im[d], re[b] - re[d], im[b] - im[d]
            return [(pr + sr, pi + si), (qr + ti, qi - tr), (pr - sr, pi - si), (qr - ti, qi + tr)]

        even, odd = four((0, 2, 4, 6)), four((1, 3, 5, 7))
        o1 = ((odd[1][0] + odd[1][1]) * root, (odd[1][1] - odd[1][0]) * root)
        o2 = (odd[2][1], -odd[2][0])
        o3 = ((odd[3][1] - odd[3][0]) * root, -(odd[3][0] + odd[3][1]) * root)
        turned = [odd[0], o1, o2, o3]
        for k in range(4):
            for sign in (0, 1):
                zr = even[k][0] - turned[k][0] if sign else even[k][0] + turned[k][0]
                zi = even[k][1] - turned[k][1] if sign else even[k][1] + turned[k][1]
                halves[k + 4 * sign, rows, 0:128] = zr.astype(BF16)
                halves[k + 4 * sign, rows, 128:256] = zi.astype(BF16)
        return carry

    lax.fori_loop(0, 8, one, 0)


def powers(halves, dft, power_k):
    def one(k, carry):
        spec = jnp.dot(halves[k], dft[k], preferred_element_type=F32)
        square = spec * spec
        total = square[:, 0:128] + square[:, 128:256]
        mean = total[0:32] + total[32:64] + total[64:96] + total[96:128]
        mean = mean * (1.0 / (FRAMES * CH))
        lanes = pl.ds(pl.multiple_of(128 * k, 128), 128)
        for m in range(8):
            moved = pltpu.roll(mean, 128 - 16 * m, 1) if m else mean
            power_k[32 * m : 32 * m + 32, lanes] = moved.astype(BF16)
        return carry

    lax.fori_loop(0, 8, one, 0, unroll=2)


def natural_order(power_k, power):
    source, lane = iota((CH, 128), 0), iota((CH, 128), 1)
    select = jnp.where(lane == source // 128 + 8 * (source % 128), 1.0, 0.0).astype(BF16)
    ordered = jnp.dot(power_k[...], select, preferred_element_type=F32)
    for m in range(8):
        power[:, 128 * m : 128 * m + 128] = ordered[32 * m : 32 * m + 32].astype(BF16)


def stack_weights(raw, rows_f32, weights):
    def one(i, carry):
        for k in range(8):
            piece = raw[k, :, pl.ds(pl.multiple_of(512 * i, 512), 512)].astype(F32)
            for m in range(4):
                start = 32 * m + 16 * (k % 2) + k // 2
                rows_f32[pl.ds(start, 4, stride=4), :] = piece[:, 128 * m : 128 * m + 128]
        for m in range(4):
            lanes = pl.ds(pl.multiple_of(512 * i + 128 * m, 128), 128)
            weights[:, lanes] = rows_f32[32 * m : 32 * m + 32, :].astype(BF16)
        return carry

    lax.fori_loop(0, 32, one, 0)


def regroup(arrived, first, out):
    lane = iota((8, 128), 1) // E_DEV
    blocks = [arrived[first + c].astype(F32) for c in range(4)]
    frames = []
    for f in range(FRAMES):
        value = None
        for c in range(4):
            shift = ((c - f) % 4) * E_DEV
            moved = pltpu.roll(blocks[c], shift, 1) if shift else blocks[c]
            value = moved if value is None else jnp.where(lane == c, moved, value)
        frames.append(value)
    out[...] = jnp.concatenate(frames, axis=0).astype(BF16)


def beams_out(total, rows, beams):
    row, col = iota((32, 128), 0), iota((32, 128), 1)
    same = jnp.where((row % 4 == (col // 4) % 4) & (col < 32), total[...], 0.0)
    folded = same + pltpu.roll(same, 124, 1) + pltpu.roll(same, 120, 1) + pltpu.roll(same, 116, 1)
    wide = folded.reshape(4, 8, 128)
    crossed = pltpu.roll(pltpu.roll(folded, 112, 1).reshape(4, 8, 128), 4, 1)
    real = iota((4, 8, 128), 1) < 4
    rows[...] = jnp.where(real, wide - crossed, wide + crossed).reshape(32, 128)
    ordered = jnp.concatenate([rows[pl.ds(k, 4, stride=8), :] for k in range(8)], axis=0)
    turned = ordered.T
    beams[0] = turned[0:4, 0:16]
    beams[1] = turned[0:4, 16:32]


def kernel(
    volt_h, delay_h, proto_h, map_h, raw_h, dft_h,
    power, beams,
    volt, delay_s, map_s, proto_v, taps_a, taps_b, coef, column, basis, wave, chosen, arrived,
    halves, dft, power_k, raw, rows_f32, weights, across_a, across_b, total, final,
    in_sem, volt_sem, shot_send, shot_recv, hop_send, hop_recv,
):
    z, xl, y = lax.axis_index("z"), lax.axis_index("xl"), lax.axis_index("y")
    xh, core = lax.axis_index("xh"), lax.axis_index("core")
    chan = xh * 2 + core
    ahead_y = [lax.rem(y + r, RING) for r in range(RING)]
    ahead_z = [lax.rem(z + r, RING) for r in range(RING)]

    small = [
        pltpu.make_async_copy(delay_h, delay_s, in_sem.at[0]),
        pltpu.make_async_copy(map_h, map_s, in_sem.at[1]),
        pltpu.make_async_copy(proto_h, proto_v, in_sem.at[2]),
    ]
    for copy in small:
        copy.start()
    chunks = []
    for g in range(2):
        for part in range(2):
            rows = pl.ds(16 * g, 16)
            chunks.append(
                pltpu.make_async_copy(volt_h.at[part, rows, :], volt.at[part, rows, :], volt_sem.at[2 * g + part])
            )
    chunks[0].start()
    later = [
        pltpu.make_async_copy(raw_h, raw, in_sem.at[3]),
        pltpu.make_async_copy(dft_h, dft, in_sem.at[4]),
    ]

    barrier = pltpu.get_barrier_semaphore()

    def hello(device):
        pl.semaphore_signal(barrier, inc=1, device_id=device, device_id_type=MESH)

    others = [lax.rem(chan + q, 4) for q in range(4)]
    for colour in range(2):
        for i in range(RING):
            for q in range(4):
                device = {"xl": colour, "xh": others[q] // 2, "core": lax.rem(others[q], 2)}
                device["z" if colour else "y"] = (ahead_z if colour else ahead_y)[i]
                if i == 0 and q == 0:
                    pl.when(xl != colour)(functools.partial(hello, device))
                else:
                    hello(device)
    for r in (1, 2, 6, 7):
        side_y = lax.rem(y + r * xl, RING)
        side_z = lax.rem(z + r * (1 - xl), RING)
        hello({"y": side_y, "z": side_z})

    for copy in small:
        copy.wait()
    for copy in chunks[1:]:
        copy.start()
    delay_column(delay_s, column)
    rotated_taps(delay_s, proto_v, taps_a, taps_b, coef)
    chosen_basis(map_s, basis)
    for g in range(2):
        for part in range(2):
            chunks[2 * g + part].wait()
            if g == 1 and part == 1:
                for copy in later:
                    copy.start()
            filter_chunk(part, g, volt, coef, column, wave)
    chosen_spectra(delay_s, map_s, basis, wave, chosen)

    pl.semaphore_wait(barrier, 2 * RING * 4 - 1 + 4)

    line = xl * 4 + chan
    mine = xl * 32 + chan
    places = [lax.rem(line + q, LINE) for q in range(LINE)]
    for i in range(RING):
        r = ORDER[i]
        shot_y = lax.rem(y + r * (1 - xl), RING)
        shot_z = lax.rem(z + r * xl, RING)
        for q in (3, 5, 2, 6, 1, 7, 4, 0):
            if i == 0 and q == 0:
                continue
            place = places[q]
            pltpu.make_async_remote_copy(
                src_ref=chosen.at[lax.rem(place, 4)],
                dst_ref=arrived.at[mine + 4 * i],
                send_sem=shot_send,
                recv_sem=shot_recv.at[xl * RING + i],
                device_id={
                    "xl": place // 4, "xh": lax.rem(place // 2, 2), "core": lax.rem(place, 2),
                    "y": shot_y, "z": shot_z,
                },
                device_id_type=MESH,
            ).start()
    arrived[mine] = chosen[chan]

    later[0].wait()
    stack_weights(raw, rows_f32, weights)
    butterflies(wave, halves)
    later[1].wait()
    powers(halves, dft, power_k)

    across = (across_a, across_b)
    aside = ("z", "y")
    ahead = (ahead_z, ahead_y)

    def shot(colour, i, count):
        return pltpu.make_async_remote_copy(
            src_ref=arrived.at[pl.ds(0, count)],
            dst_ref=arrived.at[pl.ds(colour * 32 + 4 * i, count)],
            send_sem=shot_send,
            recv_sem=shot_recv.at[colour * RING + i],
            device_id={"y": ahead_y[1]},
            device_id_type=MESH,
        )

    def ready(colour, i):
        if i:
            shot(colour, i, 4).wait_recv()
        else:
            pl.when(xl == colour)(lambda: shot(colour, i, 3).wait_recv())
            pl.when(xl != colour)(lambda: shot(colour, i, 4).wait_recv())
        regroup(arrived, colour * 32 + 4 * i, across[colour].at[0, i])

    def hop(colour, way, kind, i):
        sign = -1 if way else 1
        held = (0, 0, 2, 2)[kind] * sign % RING
        step = (1, 2, 1, 2)[kind] * sign % RING
        return pltpu.make_async_remote_copy(
            src_ref=across[colour].at[held, i],
            dst_ref=across[colour].at[(held + step) % RING, i],
            send_sem=hop_send.at[colour, way, kind],
            recv_sem=hop_recv.at[colour, way, kind, i],
            device_id={aside[colour]: ahead[colour][step]},
            device_id_type=MESH,
        )

    total[...] = jnp.zeros_like(total)

    def add(pieces):
        data, weight = [], []
        for colour, held, i in pieces:
            zz = ahead_z[(RING - (held if colour == 0 else ORDER[i])) % RING]
            yy = ahead_y[(RING - (ORDER[i] if colour == 0 else held)) % RING]
            block = (zz * 2 + colour) * RING + yy
            data.append(across[colour][held, i])
            weight.append(weights[:, pl.ds(pl.multiple_of(block * 128, 128), 128)])
        total[:, 0:32] += nt_dot(jnp.concatenate(data, axis=1), jnp.concatenate(weight, axis=1))

    for i in range(RING):
        for colour in range(2):
            ready(colour, i)
            for way in range(2):
                hop(colour, way, 1, i).start()
                hop(colour, way, 0, i).start()

    for i in range(RING):
        for colour in range(2):
            for way in range(2):
                hop(colour, way, 1, i).wait_recv()
                if i % 2 == way:
                    hop(colour, way, 3, i).start()
                hop(colour, way, 2, i).start()
    natural_order(power_k, power)
    add([(colour, 0, i) for colour in range(2) for i in range(RING)])
    for i in range(RING):
        for colour in range(2):
            for way in range(2):
                hop(colour, way, 0, i).wait_recv()
    for held in (1, 2, 6, 7):
        add([(colour, held, i) for colour in range(2) for i in range(RING)])
    pltpu.make_async_remote_copy(
        src_ref=arrived.at[pl.ds(0, 63)],
        dst_ref=arrived.at[pl.ds(0, 63)],
        send_sem=shot_send,
        recv_sem=shot_recv.at[0],
        device_id={"y": ahead_y[1]},
        device_id_type=MESH,
    ).wait_send()
    for pair in range(4):
        pieces = []
        for i in (2 * pair, 2 * pair + 1):
            for colour in range(2):
                for way in range(2):
                    hop(colour, way, 2, i).wait_recv()
                    pieces.append((colour, 5 if way else 3, i))
                    if i % 2 == way:
                        hop(colour, way, 3, i).wait_recv()
                        pieces.append((colour, 4, i))
        add(pieces)
    beams_out(total, final, beams)

    for colour in range(2):
        for way in range(2):
            for kind in range(4):
                count = 4 if kind == 3 else 8
                pltpu.make_async_remote_copy(
                    src_ref=across[colour].at[0, pl.ds(0, count)],
                    dst_ref=across[colour].at[0, pl.ds(0, count)],
                    send_sem=hop_send.at[colour, way, kind],
                    recv_sem=hop_recv.at[colour, way, kind, 0],
                    device_id={"y": ahead_y[1]},
                    device_id_type=MESH,
                ).wait_send()


def put_out(power, beams, power_h, beams_h, sem):
    copies = [pltpu.make_async_copy(power, power_h, sem.at[0]), pltpu.make_async_copy(beams, beams_h, sem.at[1])]
    for copy in copies:
        copy.start()
    for copy in copies:
        copy.wait()


def on_device(voltages, delays, prototype, subband_map, beam_weights):
    arrays = (voltages, delays, prototype, subband_map, beam_weights.reshape(8, 4, 16384), jnp.asarray(dft_blocks()))
    arrays = [pltpu.with_memory_space_constraint(array, pltpu.HBM) for array in arrays]
    any_spec = pl.BlockSpec(memory_space=pl.ANY)
    dma = pltpu.SemaphoreType.DMA
    power, beams = pl.pallas_call(
        kernel,
        out_shape=(
            jax.ShapeDtypeStruct((E_DEV, CH), BF16),
            jax.ShapeDtypeStruct((2, 4, 16), F32),
        ),
        in_specs=[any_spec] * 6,
        out_specs=(pl.BlockSpec(memory_space=pltpu.VMEM), pl.BlockSpec(memory_space=pltpu.VMEM)),
        scratch_shapes=[
            pltpu.VMEM((2, E_DEV, SAMP), BF16),
            pltpu.SMEM((E_DEV,), jnp.int32),
            pltpu.SMEM((16,), jnp.int32),
            pltpu.VMEM((TAPS, CH), BF16),
            pltpu.VMEM((128, 128), F32),
            pltpu.VMEM((128, 128), F32),
            pltpu.VMEM((128 * PAD, 128), F32),
            pltpu.VMEM((E_DEV, 128), jnp.int32),
            pltpu.VMEM((64, 2 * CH), BF16),
            pltpu.VMEM((128, 2 * CH), BF16),
            pltpu.VMEM((4, 8, 128), BF16),
            pltpu.VMEM((64, 8, 128), BF16),
            pltpu.VMEM((8, 128, 256), BF16),
            pltpu.VMEM((8, 256, 256), BF16),
            pltpu.VMEM((8 * E_DEV, CH), BF16),
            pltpu.VMEM((8, 4, 16384), BF16),
            pltpu.VMEM((128, 128), F32),
            pltpu.VMEM((32, 16384), BF16),
            pltpu.VMEM((RING, RING, 32, 128), BF16),
            pltpu.VMEM((RING, RING, 32, 128), BF16),
            pltpu.VMEM((32, 128), F32),
            pltpu.VMEM((32, 128), F32),
            dma((5,)),
            dma((4,)),
            dma,
            dma((2 * RING,)),
            dma((2, 2, 4)),
            dma((2, 2, 4, RING)),
        ],
        compiler_params=pltpu.CompilerParams(collective_id=0, has_side_effects=True, vmem_limit_bytes=48_000_000),
        name="channelize_and_beamform",
    )(*arrays)
    power, beams = pl.pallas_call(
        put_out,
        out_shape=(jax.ShapeDtypeStruct((E_DEV, CH), BF16), jax.ShapeDtypeStruct((2, 4, 16), F32)),
        in_specs=[pl.BlockSpec(memory_space=pltpu.VMEM)] * 2,
        out_specs=(pl.BlockSpec(memory_space=pltpu.HBM),) * 2,
        scratch_shapes=[dma((2,))],
        compiler_params=pltpu.CompilerParams(vmem_limit_bytes=16_000_000),
        name="put_out",
    )(power, beams)
    beams = jnp.transpose(beams, (0, 2, 1))
    return power, beams


def solution(mesh):
    finer = Mesh(mesh.devices.reshape(8, 2, 8, 2, 2), ("z", "xl", "y", "xh", "core"))
    elem, chan = ("z", "xl", "y"), ("xh", "core")
    placed = (P(None, elem + chan, None), P(elem + chan), P(), P(), P(elem, None, chan, None))
    return jax.shard_map(
        on_device,
        mesh=finer,
        in_specs=placed,
        out_specs=(P(elem + chan, None), P(None, chan, elem)),
        check_vma=False,
    )
```

```python
import functools
import math

import numpy as np
import jax
import jax.numpy as jnp
from jax import lax
from jax.experimental import pallas as pl
from jax.experimental.pallas import tpu as pltpu
from jax.sharding import Mesh
from jax.sharding import PartitionSpec as P

MESH = pl.DeviceIdType.MESH
CH, TAPS, FRAMES, E_DEV = 1024, 16, 4, 32
BLOCKS = FRAMES + TAPS - 1
SAMP = 19584
RING = 8
LINE = 8
PAD = 36
ORDER = (0, 1, 7, 2, 6, 3, 5, 4)
F32, BF16 = jnp.float32, jnp.bfloat16


def dft_blocks():
    k1 = np.arange(8)[:, None, None]
    p2 = np.arange(128)[None, :, None]
    k2 = np.arange(128)[None, None, :]
    angle = ((p2 * (k1 + 8 * k2)) % CH) * (2.0 * np.pi / CH)
    c, s = np.cos(angle), np.sin(angle)
    top = np.concatenate([c, -s], axis=2)
    low = np.concatenate([s, c], axis=2)
    return np.concatenate([top, low], axis=1).astype(jnp.bfloat16)


def iota(shape, dim):
    return lax.broadcasted_iota(jnp.int32, shape, dim)


def cos_turns(u):
    h = (u - jnp.round(u)) * math.pi
    q = h * h
    s = h * (1.0 + q * (-1.0 / 6 + q * (1.0 / 120 + q * (-1.0 / 5040 + q * (1.0 / 362880 - q * (1.0 / 39916800))))))
    return 1.0 - 2.0 * s * s


def nt_dot(a, b):
    return lax.dot_general(a, b, (((1,), (1,)), ((), ())), preferred_element_type=F32)


def rotated_taps(delay_s, proto_v, taps_a, taps_b, coef):
    taps = proto_v[...].astype(F32)
    for j in range(8):
        block = taps[:, 128 * j : 128 * j + 128]
        taps_a[pl.ds(j, TAPS, stride=8), :] = block
        taps_b[pl.ds((j + 1) % 8, TAPS, stride=8), :] = block
    lane = iota((128, 128), 1)

    def one(n, carry):
        d = delay_s[n]
        mixed = jnp.where(lane < 128 - d, taps_a[...], taps_b[...])
        coef[pl.ds(n, 128, stride=PAD), :] = pltpu.roll(mixed, d, 1)
        return carry

    lax.fori_loop(0, E_DEV, one, 0, unroll=16)


def delay_column(delay_s, column):
    row = iota((E_DEV, 128), 0)
    value = jnp.zeros((E_DEV, 128), jnp.int32)
    for n in range(E_DEV):
        value = jnp.where(row == n, delay_s[n], value)
    column[...] = value


def channel_rows(map_s, rows):
    row = iota((rows, 128), 0)
    which = ((row // 8) % 4) * 4 + row % 4
    value = jnp.zeros((rows, 128), jnp.int32)
    for s in range(16):
        value = jnp.where(which == s, map_s[s], value)
    return value.astype(F32)


def chosen_basis(map_s, basis):
    chan = channel_rows(map_s, 32) * (1.0 / CH)
    second = (iota((32, 128), 0) // 4) % 2
    of_real = jnp.where(second == 0, 0.0, 0.25)
    of_imag = jnp.where(second == 0, -0.25, 0.0)
    lane = iota((32, 128), 1)
    for j in range(8):
        turns = chan * (lane + 128 * j).astype(F32)
        a = cos_turns(turns + of_real).astype(BF16)
        b = cos_turns(turns + of_imag).astype(BF16)
        left, right = slice(128 * j, 128 * j + 128), slice(CH + 128 * j, CH + 128 * j + 128)
        basis[0:32, left] = a
        basis[0:32, right] = b
        basis[32:64, left] = b
        basis[32:64, right] = -a


def filter_block(part, g, j, special, volt, coef, column, wave):
    rows = slice(16 * g, 16 * g + 16)

    def samples(b):
        start = b * CH + 128 * j
        if not isinstance(j, int):
            start = pl.multiple_of(start, 128)
        return volt[part, rows, pl.ds(start, 128)].astype(F32)

    sums = [None] * FRAMES
    if special:
        late = iota((16, 128), 1) < column[rows, :]
        following = samples(0)
    taps = {}
    for b in range(BLOCKS):
        if special:
            now = following
            following = samples(b + 1)
            value = jnp.where(late, following, now)
        else:
            value = samples(b)
        if b < TAPS:
            start = (b * 8 + j) * PAD + 16 * g
            if not isinstance(j, int):
                start = pl.multiple_of(start, 4)
            taps[b] = coef[pl.ds(start, 16), :]
        for f in range(FRAMES):
            t = b - f
            if 0 <= t < TAPS:
                term = taps[t] * value
                sums[f] = term if sums[f] is None else sums[f] + term
    column_start = part * CH + 128 * j
    if not isinstance(j, int):
        column_start = pl.multiple_of(column_start, 128)
    for f in range(FRAMES):
        wave[pl.ds(f * E_DEV + 16 * g, 16), pl.ds(column_start, 128)] = sums[f].astype(BF16)


def filter_chunk(part, g, volt, coef, column, wave):
    filter_block(part, g, 0, True, volt, coef, column, wave)

    def one(j, carry):
        filter_block(part, g, j, False, volt, coef, column, wave)
        return carry

    lax.fori_loop(1, 8, one, 0)


def chosen_spectra(delay_s, map_s, basis, wave, chosen):
    both = nt_dot(basis[...], wave[...])
    lane = iota((32, 128), 1) % E_DEV
    delay = jnp.zeros((32, 128), jnp.int32)
    for n in range(E_DEV):
        delay = jnp.where(lane == n, delay_s[n], delay)
    turns = channel_rows(map_s, 32) * delay.astype(F32) * (1.0 / CH)
    picked = both[:32] * cos_turns(turns) + both[32:] * cos_turns(turns - 0.25)
    picked = picked * (1.0 / math.sqrt(CH))
    for c in range(4):
        chosen[c] = picked[8 * c : 8 * c + 8].astype(BF16)


def butterflies(wave, halves):
    root = math.sqrt(0.5)

    def one(i, carry):
        rows = pl.ds(pl.multiple_of(16 * i, 16), 16)
        re = [wave[rows, 128 * j : 128 * j + 128].astype(F32) for j in range(8)]
        im = [wave[rows, CH + 128 * j : CH + 128 * j + 128].astype(F32) for j in range(8)]

        def four(ids):
            a, b, c, d = ids
            pr, pi, qr, qi = re[a] + re[c], im[a] + im[c], re[a] - re[c], im[a] - im[c]
            sr, si, tr, ti = re[b] + re[d], im[b] + im[d], re[b] - re[d], im[b] - im[d]
            return [(pr + sr, pi + si), (qr + ti, qi - tr), (pr - sr, pi - si), (qr - ti, qi + tr)]

        even, odd = four((0, 2, 4, 6)), four((1, 3, 5, 7))
        o1 = ((odd[1][0] + odd[1][1]) * root, (odd[1][1] - odd[1][0]) * root)
        o2 = (odd[2][1], -odd[2][0])
        o3 = ((odd[3][1] - odd[3][0]) * root, -(odd[3][0] + odd[3][1]) * root)
        turned = [odd[0], o1, o2, o3]
        for k in range(4):
            for sign in (0, 1):
                zr = even[k][0] - turned[k][0] if sign else even[k][0] + turned[k][0]
                zi = even[k][1] - turned[k][1] if sign else even[k][1] + turned[k][1]
                halves[k + 4 * sign, rows, 0:128] = zr.astype(BF16)
                halves[k + 4 * sign, rows, 128:256] = zi.astype(BF16)
        return carry

    lax.fori_loop(0, 8, one, 0)


def powers(halves, dft, power_k):
    def one(k, carry):
        spec = jnp.dot(halves[k], dft[k], preferred_element_type=F32)
        square = spec * spec
        total = square[:, 0:128] + square[:, 128:256]
        mean = total[0:32] + total[32:64] + total[64:96] + total[96:128]
        mean = mean * (1.0 / (FRAMES * CH))
        lanes = pl.ds(pl.multiple_of(128 * k, 128), 128)
        for m in range(8):
            moved = pltpu.roll(mean, 128 - 16 * m, 1) if m else mean
            power_k[32 * m : 32 * m + 32, lanes] = moved.astype(BF16)
        return carry

    lax.fori_loop(0, 8, one, 0, unroll=2)


def natural_order(power_k, power):
    source, lane = iota((CH, 128), 0), iota((CH, 128), 1)
    select = jnp.where(lane == source // 128 + 8 * (source % 128), 1.0, 0.0).astype(BF16)
    ordered = jnp.dot(power_k[...], select, preferred_element_type=F32)
    for m in range(8):
        power[:, 128 * m : 128 * m + 128] = ordered[32 * m : 32 * m + 32].astype(BF16)


def stack_weights(raw, rows_f32, weights):
    def one(i, carry):
        for k in range(8):
            piece = raw[k, :, pl.ds(pl.multiple_of(512 * i, 512), 512)].astype(F32)
            for m in range(4):
                start = 32 * m + 16 * (k % 2) + k // 2
                rows_f32[pl.ds(start, 4, stride=4), :] = piece[:, 128 * m : 128 * m + 128]
        for m in range(4):
            lanes = pl.ds(pl.multiple_of(512 * i + 128 * m, 128), 128)
            weights[:, lanes] = rows_f32[32 * m : 32 * m + 32, :].astype(BF16)
        return carry

    lax.fori_loop(0, 32, one, 0)


def regroup(arrived, first, out):
    lane = iota((8, 128), 1) // E_DEV
    blocks = [arrived[first + c].astype(F32) for c in range(4)]
    frames = []
    for f in range(FRAMES):
        value = None
        for c in range(4):
            shift = ((c - f) % 4) * E_DEV
            moved = pltpu.roll(blocks[c], shift, 1) if shift else blocks[c]
            value = moved if value is None else jnp.where(lane == c, moved, value)
        frames.append(value)
    out[...] = jnp.concatenate(frames, axis=0).astype(BF16)


def beams_out(total, rows, beams):
    row, col = iota((32, 128), 0), iota((32, 128), 1)
    same = jnp.where((row % 4 == (col // 4) % 4) & (col < 32), total[...], 0.0)
    folded = same + pltpu.roll(same, 124, 1) + pltpu.roll(same, 120, 1) + pltpu.roll(same, 116, 1)
    wide = folded.reshape(4, 8, 128)
    crossed = pltpu.roll(pltpu.roll(folded, 112, 1).reshape(4, 8, 128), 4, 1)
    real = iota((4, 8, 128), 1) < 4
    rows[...] = jnp.where(real, wide - crossed, wide + crossed).reshape(32, 128)
    ordered = jnp.concatenate([rows[pl.ds(k, 4, stride=8), :] for k in range(8)], axis=0)
    turned = ordered.T
    beams[0] = turned[0:4, 0:16]
    beams[1] = turned[0:4, 16:32]


def kernel(
    volt_h, delay_h, proto_h, map_h, raw_h, dft_h,
    power, beams,
    volt, delay_s, map_s, proto_v, taps_a, taps_b, coef, column, basis, wave, chosen, arrived,
    halves, dft, power_k, raw, rows_f32, weights, across_a, across_b, total, final,
    in_sem, volt_sem, shot_send, shot_recv, hop_send, hop_recv,
):
    z, xl, y = lax.axis_index("z"), lax.axis_index("xl"), lax.axis_index("y")
    xh, core = lax.axis_index("xh"), lax.axis_index("core")
    chan = xh * 2 + core
    ahead_y = [lax.rem(y + r, RING) for r in range(RING)]
    ahead_z = [lax.rem(z + r, RING) for r in range(RING)]

    small = [
        pltpu.make_async_copy(delay_h, delay_s, in_sem.at[0]),
        pltpu.make_async_copy(map_h, map_s, in_sem.at[1]),
        pltpu.make_async_copy(proto_h, proto_v, in_sem.at[2]),
    ]
    for copy in small:
        copy.start()
    chunks = []
    for g in range(2):
        for part in range(2):
            rows = pl.ds(16 * g, 16)
            chunks.append(
                pltpu.make_async_copy(volt_h.at[part, rows, :], volt.at[part, rows, :], volt_sem.at[2 * g + part])
            )
    chunks[0].start()
    later = [
        pltpu.make_async_copy(raw_h, raw, in_sem.at[3]),
        pltpu.make_async_copy(dft_h, dft, in_sem.at[4]),
    ]

    barrier = pltpu.get_barrier_semaphore()

    def hello(device):
        pl.semaphore_signal(barrier, inc=1, device_id=device, device_id_type=MESH)

    others = [lax.rem(chan + q, 4) for q in range(4)]
    for i in range(RING - 1, -1, -1):
        for colour in range(2):
            for q in (2, 3, 1, 0):
                device = {"xl": colour, "xh": others[q] // 2, "core": lax.rem(others[q], 2)}
                device["z" if colour else "y"] = (ahead_z if colour else ahead_y)[ORDER[i]]
                if i == 0 and q == 0:
                    pl.when(xl != colour)(functools.partial(hello, device))
                else:
                    hello(device)
    for r in (2, 6, 1, 7):
        side_y = lax.rem(y + r * xl, RING)
        side_z = lax.rem(z + r * (1 - xl), RING)
        hello({"y": side_y, "z": side_z})

    for copy in small:
        copy.wait()
    for copy in chunks[1:]:
        copy.start()
    delay_column(delay_s, column)
    rotated_taps(delay_s, proto_v, taps_a, taps_b, coef)
    chosen_basis(map_s, basis)
    for g in range(2):
        for part in range(2):
            chunks[2 * g + part].wait()
            if g == 1 and part == 1:
                for copy in later:
                    copy.start()
            filter_chunk(part, g, volt, coef, column, wave)
    chosen_spectra(delay_s, map_s, basis, wave, chosen)

    pl.semaphore_wait(barrier, 2 * RING * 4 - 1 + 4)

    line = xl * 4 + chan
    mine = xl * 32 + chan
    places = [lax.rem(line + q, LINE) for q in range(LINE)]
    for i in range(RING):
        r = ORDER[i]
        shot_y = lax.rem(y + r * (1 - xl), RING)
        shot_z = lax.rem(z + r * xl, RING)
        for q in (3, 5, 2, 6, 1, 7, 4, 0):
            if i == 0 and q == 0:
                continue
            place = places[q]
            pltpu.make_async_remote_copy(
                src_ref=chosen.at[lax.rem(place, 4)],
                dst_ref=arrived.at[mine + 4 * i],
                send_sem=shot_send,
                recv_sem=shot_recv.at[xl * RING + i],
                device_id={
                    "xl": place // 4, "xh": lax.rem(place // 2, 2), "core": lax.rem(place, 2),
                    "y": shot_y, "z": shot_z,
                },
                device_id_type=MESH,
            ).start()
    arrived[mine] = chosen[chan]

    later[0].wait()
    stack_weights(raw, rows_f32, weights)
    butterflies(wave, halves)
    later[1].wait()
    powers(halves, dft, power_k)

    across = (across_a, across_b)
    aside = ("z", "y")
    ahead = (ahead_z, ahead_y)

    def shot(colour, i, count):
        return pltpu.make_async_remote_copy(
            src_ref=arrived.at[pl.ds(0, count)],
            dst_ref=arrived.at[pl.ds(colour * 32 + 4 * i, count)],
            send_sem=shot_send,
            recv_sem=shot_recv.at[colour * RING + i],
            device_id={"y": ahead_y[1]},
            device_id_type=MESH,
        )

    def ready(colour, i):
        if i:
            shot(colour, i, 4).wait_recv()
        else:
            pl.when(xl == colour)(lambda: shot(colour, i, 3).wait_recv())
            pl.when(xl != colour)(lambda: shot(colour, i, 4).wait_recv())
        regroup(arrived, colour * 32 + 4 * i, across[colour].at[0, i])

    def hop(colour, way, kind, i):
        sign = -1 if way else 1
        held = (0, 0, 2, 2)[kind] * sign % RING
        step = (1, 2, 1, 2)[kind] * sign % RING
        return pltpu.make_async_remote_copy(
            src_ref=across[colour].at[held, i],
            dst_ref=across[colour].at[(held + step) % RING, i],
            send_sem=hop_send.at[colour, way, kind],
            recv_sem=hop_recv.at[colour, way, kind, i],
            device_id={aside[colour]: ahead[colour][step]},
            device_id_type=MESH,
        )

    total[...] = jnp.zeros_like(total)

    def add(pieces):
        data, weight = [], []
        for colour, held, i in pieces:
            zz = ahead_z[(RING - (held if colour == 0 else ORDER[i])) % RING]
            yy = ahead_y[(RING - (ORDER[i] if colour == 0 else held)) % RING]
            block = (zz * 2 + colour) * RING + yy
            data.append(across[colour][held, i])
            weight.append(weights[:, pl.ds(pl.multiple_of(block * 128, 128), 128)])
        total[:, 0:32] += nt_dot(jnp.concatenate(data, axis=1), jnp.concatenate(weight, axis=1))

    for i in range(RING):
        for colour in range(2):
            ready(colour, i)
            for way in range(2):
                hop(colour, way, 1, i).start()
                hop(colour, way, 0, i).start()

    def near(pair):
        pieces = []
        for i in (2 * pair, 2 * pair + 1):
            for colour in range(2):
                for way in range(2):
                    hop(colour, way, 0, i).wait_recv()
                pieces += [(colour, held, i) for held in (0, 1, 2, 6, 7)]
        add(pieces)

    for i in range(RING):
        for colour in range(2):
            for way in range(2):
                hop(colour, way, 1, i).wait_recv()
                if i % 2 == way:
                    hop(colour, way, 3, i).start()
                hop(colour, way, 2, i).start()
        if i % 2:
            near(i // 2)
    natural_order(power_k, power)
    pltpu.make_async_remote_copy(
        src_ref=arrived.at[pl.ds(0, 63)],
        dst_ref=arrived.at[pl.ds(0, 63)],
        send_sem=shot_send,
        recv_sem=shot_recv.at[0],
        device_id={"y": ahead_y[1]},
        device_id_type=MESH,
    ).wait_send()
    for pair in range(4):
        pieces = []
        for i in (2 * pair, 2 * pair + 1):
            for colour in range(2):
                for way in range(2):
                    hop(colour, way, 2, i).wait_recv()
                    pieces.append((colour, 5 if way else 3, i))
                    if i % 2 == way:
                        hop(colour, way, 3, i).wait_recv()
                        pieces.append((colour, 4, i))
        add(pieces)
    beams_out(total, final, beams)

    for colour in range(2):
        for way in range(2):
            for kind in range(4):
                count = 4 if kind == 3 else 8
                pltpu.make_async_remote_copy(
                    src_ref=across[colour].at[0, pl.ds(0, count)],
                    dst_ref=across[colour].at[0, pl.ds(0, count)],
                    send_sem=hop_send.at[colour, way, kind],
                    recv_sem=hop_recv.at[colour, way, kind, 0],
                    device_id={"y": ahead_y[1]},
                    device_id_type=MESH,
                ).wait_send()


def put_out(power, beams, power_h, beams_h, sem):
    copies = [pltpu.make_async_copy(power, power_h, sem.at[0]), pltpu.make_async_copy(beams, beams_h, sem.at[1])]
    for copy in copies:
        copy.start()
    for copy in copies:
        copy.wait()


def on_device(voltages, delays, prototype, subband_map, beam_weights):
    arrays = (voltages, delays, prototype, subband_map, beam_weights.reshape(8, 4, 16384), jnp.asarray(dft_blocks()))
    arrays = [pltpu.with_memory_space_constraint(array, pltpu.HBM) for array in arrays]
    any_spec = pl.BlockSpec(memory_space=pl.ANY)
    dma = pltpu.SemaphoreType.DMA
    power, beams = pl.pallas_call(
        kernel,
        out_shape=(
            jax.ShapeDtypeStruct((E_DEV, CH), BF16),
            jax.ShapeDtypeStruct((2, 4, 16), F32),
        ),
        in_specs=[any_spec] * 6,
        out_specs=(pl.BlockSpec(memory_space=pltpu.VMEM), pl.BlockSpec(memory_space=pltpu.VMEM)),
        scratch_shapes=[
            pltpu.VMEM((2, E_DEV, SAMP), BF16),
            pltpu.SMEM((E_DEV,), jnp.int32),
            pltpu.SMEM((16,), jnp.int32),
            pltpu.VMEM((TAPS, CH), BF16),
            pltpu.VMEM((128, 128), F32),
            pltpu.VMEM((128, 128), F32),
            pltpu.VMEM((128 * PAD, 128), F32),
            pltpu.VMEM((E_DEV, 128), jnp.int32),
            pltpu.VMEM((64, 2 * CH), BF16),
            pltpu.VMEM((128, 2 * CH), BF16),
            pltpu.VMEM((4, 8, 128), BF16),
            pltpu.VMEM((64, 8, 128), BF16),
            pltpu.VMEM((8, 128, 256), BF16),
            pltpu.VMEM((8, 256, 256), BF16),
            pltpu.VMEM((8 * E_DEV, CH), BF16),
            pltpu.VMEM((8, 4, 16384), BF16),
            pltpu.VMEM((128, 128), F32),
            pltpu.VMEM((32, 16384), BF16),
            pltpu.VMEM((RING, RING, 32, 128), BF16),
            pltpu.VMEM((RING, RING, 32, 128), BF16),
            pltpu.VMEM((32, 128), F32),
            pltpu.VMEM((32, 128), F32),
            dma((5,)),
            dma((4,)),
            dma,
            dma((2 * RING,)),
            dma((2, 2, 4)),
            dma((2, 2, 4, RING)),
        ],
        compiler_params=pltpu.CompilerParams(collective_id=0, has_side_effects=True, vmem_limit_bytes=48_000_000),
        name="channelize_and_beamform",
    )(*arrays)
    power, beams = pl.pallas_call(
        put_out,
        out_shape=(jax.ShapeDtypeStruct((E_DEV, CH), BF16), jax.ShapeDtypeStruct((2, 4, 16), F32)),
        in_specs=[pl.BlockSpec(memory_space=pltpu.VMEM)] * 2,
        out_specs=(pl.BlockSpec(memory_space=pltpu.HBM),) * 2,
        scratch_shapes=[dma((2,))],
        compiler_params=pltpu.CompilerParams(vmem_limit_bytes=16_000_000),
        name="put_out",
    )(power, beams)
    beams = jnp.transpose(beams, (0, 2, 1))
    return power, beams


def solution(mesh):
    finer = Mesh(mesh.devices.reshape(8, 2, 8, 2, 2), ("z", "xl", "y", "xh", "core"))
    elem, chan = ("z", "xl", "y"), ("xh", "core")
    placed = (P(None, elem + chan, None), P(elem + chan), P(), P(), P(elem, None, chan, None))
    return jax.shard_map(
        on_device,
        mesh=finer,
        in_specs=placed,
        out_specs=(P(elem + chan, None), P(None, chan, elem)),
        check_vma=False,
    )
```

```python
import functools
import math

import numpy as np
import jax
import jax.numpy as jnp
from jax import lax
from jax.experimental import pallas as pl
from jax.experimental.pallas import tpu as pltpu
from jax.sharding import Mesh
from jax.sharding import PartitionSpec as P

MESH = pl.DeviceIdType.MESH
CH, TAPS, FRAMES, E_DEV = 1024, 16, 4, 32
BLOCKS = FRAMES + TAPS - 1
SAMP = 19584
RING = 8
LINE = 8
PAD = 36
ORDER = (0, 1, 7, 2, 6, 3, 5, 4)
F32, BF16 = jnp.float32, jnp.bfloat16


def dft_blocks():
    k1 = np.arange(8)[:, None, None]
    p2 = np.arange(128)[None, :, None]
    k2 = np.arange(128)[None, None, :]
    angle = ((p2 * (k1 + 8 * k2)) % CH) * (2.0 * np.pi / CH)
    c, s = np.cos(angle), np.sin(angle)
    top = np.concatenate([c, -s], axis=2)
    low = np.concatenate([s, c], axis=2)
    return np.concatenate([top, low], axis=1).astype(jnp.bfloat16)


def iota(shape, dim):
    return lax.broadcasted_iota(jnp.int32, shape, dim)


def cos_turns(u):
    h = (u - jnp.round(u)) * math.pi
    q = h * h
    s = h * (1.0 + q * (-1.0 / 6 + q * (1.0 / 120 + q * (-1.0 / 5040 + q * (1.0 / 362880 - q * (1.0 / 39916800))))))
    return 1.0 - 2.0 * s * s


def nt_dot(a, b):
    return lax.dot_general(a, b, (((1,), (1,)), ((), ())), preferred_element_type=F32)


def rotated_taps(delay_s, proto_v, taps_a, taps_b, coef):
    taps = proto_v[...].astype(F32)
    for j in range(8):
        block = taps[:, 128 * j : 128 * j + 128]
        taps_a[pl.ds(j, TAPS, stride=8), :] = block
        taps_b[pl.ds((j + 1) % 8, TAPS, stride=8), :] = block
    lane = iota((128, 128), 1)

    def one(n, carry):
        d = delay_s[n]
        mixed = jnp.where(lane < 128 - d, taps_a[...], taps_b[...])
        coef[pl.ds(n, 128, stride=PAD), :] = pltpu.roll(mixed, d, 1)
        return carry

    lax.fori_loop(0, E_DEV, one, 0, unroll=16)


def delay_column(delay_s, column):
    row = iota((E_DEV, 128), 0)
    value = jnp.zeros((E_DEV, 128), jnp.int32)
    for n in range(E_DEV):
        value = jnp.where(row == n, delay_s[n], value)
    column[...] = value


def channel_rows(map_s, rows):
    row = iota((rows, 128), 0)
    which = ((row // 8) % 4) * 4 + row % 4
    value = jnp.zeros((rows, 128), jnp.int32)
    for s in range(16):
        value = jnp.where(which == s, map_s[s], value)
    return value.astype(F32)


def chosen_basis(map_s, basis):
    chan = channel_rows(map_s, 32) * (1.0 / CH)
    second = (iota((32, 128), 0) // 4) % 2
    of_real = jnp.where(second == 0, 0.0, 0.25)
    of_imag = jnp.where(second == 0, -0.25, 0.0)
    lane = iota((32, 128), 1)
    for j in range(8):
        turns = chan * (lane + 128 * j).astype(F32)
        a = cos_turns(turns + of_real).astype(BF16)
        b = cos_turns(turns + of_imag).astype(BF16)
        left, right = slice(128 * j, 128 * j + 128), slice(CH + 128 * j, CH + 128 * j + 128)
        basis[0:32, left] = a
        basis[0:32, right] = b
        basis[32:64, left] = b
        basis[32:64, right] = -a


def filter_block(part, g, j, special, volt, coef, column, wave):
    rows = slice(16 * g, 16 * g + 16)

    def samples(b):
        start = b * CH + 128 * j
        if not isinstance(j, int):
            start = pl.multiple_of(start, 128)
        return volt[part, rows, pl.ds(start, 128)].astype(F32)

    sums = [None] * FRAMES
    if special:
        late = iota((16, 128), 1) < column[rows, :]
        following = samples(0)
    taps = {}
    for b in range(BLOCKS):
        if special:
            now = following
            following = samples(b + 1)
            value = jnp.where(late, following, now)
        else:
            value = samples(b)
        if b < TAPS:
            start = (b * 8 + j) * PAD + 16 * g
            if not isinstance(j, int):
                start = pl.multiple_of(start, 4)
            taps[b] = coef[pl.ds(start, 16), :]
        for f in range(FRAMES):
            t = b - f
            if 0 <= t < TAPS:
                term = taps[t] * value
                sums[f] = term if sums[f] is None else sums[f] + term
    column_start = part * CH + 128 * j
    if not isinstance(j, int):
        column_start = pl.multiple_of(column_start, 128)
    for f in range(FRAMES):
        wave[pl.ds(f * E_DEV + 16 * g, 16), pl.ds(column_start, 128)] = sums[f].astype(BF16)


def filter_chunk(part, g, volt, coef, column, wave):
    filter_block(part, g, 0, True, volt, coef, column, wave)

    def one(j, carry):
        filter_block(part, g, j, False, volt, coef, column, wave)
        return carry

    lax.fori_loop(1, 8, one, 0)


def chosen_spectra(delay_s, map_s, basis, wave, chosen):
    both = nt_dot(basis[...], wave[...])
    lane = iota((32, 128), 1) % E_DEV
    delay = jnp.zeros((32, 128), jnp.int32)
    for n in range(E_DEV):
        delay = jnp.where(lane == n, delay_s[n], delay)
    turns = channel_rows(map_s, 32) * delay.astype(F32) * (1.0 / CH)
    picked = both[:32] * cos_turns(turns) + both[32:] * cos_turns(turns - 0.25)
    picked = picked * (1.0 / math.sqrt(CH))
    for c in range(4):
        chosen[c] = picked[8 * c : 8 * c + 8].astype(BF16)


def butterflies(wave, halves):
    root = math.sqrt(0.5)

    def one(i, carry):
        rows = pl.ds(pl.multiple_of(16 * i, 16), 16)
        re = [wave[rows, 128 * j : 128 * j + 128].astype(F32) for j in range(8)]
        im = [wave[rows, CH + 128 * j : CH + 128 * j + 128].astype(F32) for j in range(8)]

        def four(ids):
            a, b, c, d = ids
            pr, pi, qr, qi = re[a] + re[c], im[a] + im[c], re[a] - re[c], im[a] - im[c]
            sr, si, tr, ti = re[b] + re[d], im[b] + im[d], re[b] - re[d], im[b] - im[d]
            return [(pr + sr, pi + si), (qr + ti, qi - tr), (pr - sr, pi - si), (qr - ti, qi + tr)]

        even, odd = four((0, 2, 4, 6)), four((1, 3, 5, 7))
        o1 = ((odd[1][0] + odd[1][1]) * root, (odd[1][1] - odd[1][0]) * root)
        o2 = (odd[2][1], -odd[2][0])
        o3 = ((odd[3][1] - odd[3][0]) * root, -(odd[3][0] + odd[3][1]) * root)
        turned = [odd[0], o1, o2, o3]
        for k in range(4):
            for sign in (0, 1):
                zr = even[k][0] - turned[k][0] if sign else even[k][0] + turned[k][0]
                zi = even[k][1] - turned[k][1] if sign else even[k][1] + turned[k][1]
                halves[k + 4 * sign, rows, 0:128] = zr.astype(BF16)
                halves[k + 4 * sign, rows, 128:256] = zi.astype(BF16)
        return carry

    lax.fori_loop(0, 8, one, 0)


def powers(halves, dft, power_k):
    def one(k, carry):
        spec = jnp.dot(halves[k], dft[k], preferred_element_type=F32)
        square = spec * spec
        total = square[:, 0:128] + square[:, 128:256]
        mean = total[0:32] + total[32:64] + total[64:96] + total[96:128]
        mean = mean * (1.0 / (FRAMES * CH))
        lanes = pl.ds(pl.multiple_of(128 * k, 128), 128)
        for m in range(8):
            moved = pltpu.roll(mean, 128 - 16 * m, 1) if m else mean
            power_k[32 * m : 32 * m + 32, lanes] = moved.astype(BF16)
        return carry

    lax.fori_loop(0, 8, one, 0, unroll=2)


def natural_order(power_k, power):
    source, lane = iota((CH, 128), 0), iota((CH, 128), 1)
    select = jnp.where(lane == source // 128 + 8 * (source % 128), 1.0, 0.0).astype(BF16)
    ordered = jnp.dot(power_k[...], select, preferred_element_type=F32)
    for m in range(8):
        power[:, 128 * m : 128 * m + 128] = ordered[32 * m : 32 * m + 32].astype(BF16)


def stack_weights(raw, rows_f32, weights):
    def one(i, carry):
        for k in range(8):
            piece = raw[k, :, pl.ds(pl.multiple_of(512 * i, 512), 512)].astype(F32)
            for m in range(4):
                start = 32 * m + 16 * (k % 2) + k // 2
                rows_f32[pl.ds(start, 4, stride=4), :] = piece[:, 128 * m : 128 * m + 128]
        for m in range(4):
            lanes = pl.ds(pl.multiple_of(512 * i + 128 * m, 128), 128)
            weights[:, lanes] = rows_f32[32 * m : 32 * m + 32, :].astype(BF16)
        return carry

    lax.fori_loop(0, 32, one, 0)


def regroup(arrived, first, out):
    lane = iota((8, 128), 1) // E_DEV
    blocks = [arrived[first + c].astype(F32) for c in range(4)]
    frames = []
    for f in range(FRAMES):
        value = None
        for c in range(4):
            shift = ((c - f) % 4) * E_DEV
            moved = pltpu.roll(blocks[c], shift, 1) if shift else blocks[c]
            value = moved if value is None else jnp.where(lane == c, moved, value)
        frames.append(value)
    out[...] = jnp.concatenate(frames, axis=0).astype(BF16)


def beams_out(total, rows, beams):
    row, col = iota((32, 128), 0), iota((32, 128), 1)
    same = jnp.where((row % 4 == (col // 4) % 4) & (col < 32), total[...], 0.0)
    folded = same + pltpu.roll(same, 124, 1) + pltpu.roll(same, 120, 1) + pltpu.roll(same, 116, 1)
    wide = folded.reshape(4, 8, 128)
    crossed = pltpu.roll(pltpu.roll(folded, 112, 1).reshape(4, 8, 128), 4, 1)
    real = iota((4, 8, 128), 1) < 4
    rows[...] = jnp.where(real, wide - crossed, wide + crossed).reshape(32, 128)
    ordered = jnp.concatenate([rows[pl.ds(k, 4, stride=8), :] for k in range(8)], axis=0)
    turned = ordered.T
    beams[0] = turned[0:4, 0:16]
    beams[1] = turned[0:4, 16:32]


def kernel(
    volt_h, delay_h, proto_h, map_h, raw_h, dft_h,
    power, beams,
    volt, delay_s, map_s, proto_v, taps_a, taps_b, coef, column, basis, wave, chosen, arrived,
    halves, dft, power_k, raw, rows_f32, weights, across_a, across_b, total, final,
    in_sem, volt_sem, shot_send, shot_recv, hop_send, hop_recv,
):
    z, xl, y = lax.axis_index("z"), lax.axis_index("xl"), lax.axis_index("y")
    xh, core = lax.axis_index("xh"), lax.axis_index("core")
    chan = xh * 2 + core
    ahead_y = [lax.rem(y + r, RING) for r in range(RING)]
    ahead_z = [lax.rem(z + r, RING) for r in range(RING)]

    small = [
        pltpu.make_async_copy(delay_h, delay_s, in_sem.at[0]),
        pltpu.make_async_copy(map_h, map_s, in_sem.at[1]),
        pltpu.make_async_copy(proto_h, proto_v, in_sem.at[2]),
    ]
    for copy in small:
        copy.start()
    chunks = []
    for g in range(2):
        for part in range(2):
            rows = pl.ds(16 * g, 16)
            chunks.append(
                pltpu.make_async_copy(volt_h.at[part, rows, :], volt.at[part, rows, :], volt_sem.at[2 * g + part])
            )
    chunks[0].start()
    later = [
        pltpu.make_async_copy(raw_h, raw, in_sem.at[3]),
        pltpu.make_async_copy(dft_h, dft, in_sem.at[4]),
    ]

    barrier = pltpu.get_barrier_semaphore()

    def hello(device):
        pl.semaphore_signal(barrier, inc=1, device_id=device, device_id_type=MESH)

    others = [lax.rem(chan + q, 4) for q in range(4)]
    for i in range(RING - 1, -1, -1):
        for colour in range(2):
            for q in (2, 3, 1, 0):
                device = {"xl": colour, "xh": others[q] // 2, "core": lax.rem(others[q], 2)}
                device["z" if colour else "y"] = (ahead_z if colour else ahead_y)[ORDER[i]]
                if i == 0 and q == 0:
                    pl.when(xl != colour)(functools.partial(hello, device))
                else:
                    hello(device)
    for r in (2, 6, 1, 7):
        side_y = lax.rem(y + r * xl, RING)
        side_z = lax.rem(z + r * (1 - xl), RING)
        hello({"y": side_y, "z": side_z})

    for copy in small:
        copy.wait()
    for copy in chunks[1:]:
        copy.start()
    delay_column(delay_s, column)
    rotated_taps(delay_s, proto_v, taps_a, taps_b, coef)
    chosen_basis(map_s, basis)
    for g in range(2):
        for part in range(2):
            chunks[2 * g + part].wait()
            if g == 1 and part == 1:
                for copy in later:
                    copy.start()
            filter_chunk(part, g, volt, coef, column, wave)
    chosen_spectra(delay_s, map_s, basis, wave, chosen)

    pl.semaphore_wait(barrier, 2 * RING * 4 - 1 + 4)

    line = xl * 4 + chan
    mine = xl * 32 + chan
    places = [lax.rem(line + q, LINE) for q in range(LINE)]
    for i in (7, 0, 1, 2, 3, 4, 5, 6):
        r = ORDER[i]
        shot_y = lax.rem(y + r * (1 - xl), RING)
        shot_z = lax.rem(z + r * xl, RING)
        for q in (3, 5, 2, 6, 1, 7, 4, 0):
            if i == 0 and q == 0:
                continue
            place = places[q]
            pltpu.make_async_remote_copy(
                src_ref=chosen.at[lax.rem(place, 4)],
                dst_ref=arrived.at[mine + 4 * i],
                send_sem=shot_send,
                recv_sem=shot_recv.at[xl * RING + i],
                device_id={
                    "xl": place // 4, "xh": lax.rem(place // 2, 2), "core": lax.rem(place, 2),
                    "y": shot_y, "z": shot_z,
                },
                device_id_type=MESH,
            ).start()
    arrived[mine] = chosen[chan]

    later[0].wait()
    stack_weights(raw, rows_f32, weights)
    butterflies(wave, halves)
    later[1].wait()
    powers(halves, dft, power_k)

    across = (across_a, across_b)
    aside = ("z", "y")
    ahead = (ahead_z, ahead_y)

    def shot(colour, i, count):
        return pltpu.make_async_remote_copy(
            src_ref=arrived.at[pl.ds(0, count)],
            dst_ref=arrived.at[pl.ds(colour * 32 + 4 * i, count)],
            send_sem=shot_send,
            recv_sem=shot_recv.at[colour * RING + i],
            device_id={"y": ahead_y[1]},
            device_id_type=MESH,
        )

    def ready(colour, i):
        if i:
            shot(colour, i, 4).wait_recv()
        else:
            pl.when(xl == colour)(lambda: shot(colour, i, 3).wait_recv())
            pl.when(xl != colour)(lambda: shot(colour, i, 4).wait_recv())
        regroup(arrived, colour * 32 + 4 * i, across[colour].at[0, i])

    def hop(colour, way, kind, i):
        sign = -1 if way else 1
        held = (0, 0, 2, 2)[kind] * sign % RING
        step = (1, 2, 1, 2)[kind] * sign % RING
        return pltpu.make_async_remote_copy(
            src_ref=across[colour].at[held, i],
            dst_ref=across[colour].at[(held + step) % RING, i],
            send_sem=hop_send.at[colour, way, kind],
            recv_sem=hop_recv.at[colour, way, kind, i],
            device_id={aside[colour]: ahead[colour][step]},
            device_id_type=MESH,
        )

    total[...] = jnp.zeros_like(total)

    def add(pieces):
        data, weight = [], []
        for colour, held, i in pieces:
            zz = ahead_z[(RING - (held if colour == 0 else ORDER[i])) % RING]
            yy = ahead_y[(RING - (ORDER[i] if colour == 0 else held)) % RING]
            block = (zz * 2 + colour) * RING + yy
            data.append(across[colour][held, i])
            weight.append(weights[:, pl.ds(pl.multiple_of(block * 128, 128), 128)])
        total[:, 0:32] += nt_dot(jnp.concatenate(data, axis=1), jnp.concatenate(weight, axis=1))

    for i in range(RING):
        for colour in range(2):
            ready(colour, i)
            for way in range(2):
                hop(colour, way, 1, i).start()
                hop(colour, way, 0, i).start()

    def near(pair):
        pieces = []
        for i in (2 * pair, 2 * pair + 1):
            for colour in range(2):
                for way in range(2):
                    hop(colour, way, 0, i).wait_recv()
                pieces += [(colour, held, i) for held in (0, 1, 2, 6, 7)]
        add(pieces)

    for i in range(RING):
        for colour in range(2):
            for way in range(2):
                hop(colour, way, 1, i).wait_recv()
                if i % 2 == way:
                    hop(colour, way, 3, i).start()
                hop(colour, way, 2, i).start()
        if i % 2:
            near(i // 2)
    natural_order(power_k, power)
    pltpu.make_async_remote_copy(
        src_ref=arrived.at[pl.ds(0, 63)],
        dst_ref=arrived.at[pl.ds(0, 63)],
        send_sem=shot_send,
        recv_sem=shot_recv.at[0],
        device_id={"y": ahead_y[1]},
        device_id_type=MESH,
    ).wait_send()
    for pair in range(4):
        pieces = []
        for i in (2 * pair, 2 * pair + 1):
            for colour in range(2):
                for way in range(2):
                    hop(colour, way, 2, i).wait_recv()
                    pieces.append((colour, 5 if way else 3, i))
                    if i % 2 == way:
                        hop(colour, way, 3, i).wait_recv()
                        pieces.append((colour, 4, i))
        add(pieces)
    beams_out(total, final, beams)

    for colour in range(2):
        for way in range(2):
            for kind in range(4):
                count = 4 if kind == 3 else 8
                pltpu.make_async_remote_copy(
                    src_ref=across[colour].at[0, pl.ds(0, count)],
                    dst_ref=across[colour].at[0, pl.ds(0, count)],
                    send_sem=hop_send.at[colour, way, kind],
                    recv_sem=hop_recv.at[colour, way, kind, 0],
                    device_id={"y": ahead_y[1]},
                    device_id_type=MESH,
                ).wait_send()


def put_out(power, beams, power_h, beams_h, sem):
    copies = [pltpu.make_async_copy(power, power_h, sem.at[0]), pltpu.make_async_copy(beams, beams_h, sem.at[1])]
    for copy in copies:
        copy.start()
    for copy in copies:
        copy.wait()


def on_device(voltages, delays, prototype, subband_map, beam_weights):
    arrays = (voltages, delays, prototype, subband_map, beam_weights.reshape(8, 4, 16384), jnp.asarray(dft_blocks()))
    arrays = [pltpu.with_memory_space_constraint(array, pltpu.HBM) for array in arrays]
    any_spec = pl.BlockSpec(memory_space=pl.ANY)
    dma = pltpu.SemaphoreType.DMA
    power, beams = pl.pallas_call(
        kernel,
        out_shape=(
            jax.ShapeDtypeStruct((E_DEV, CH), BF16),
            jax.ShapeDtypeStruct((2, 4, 16), F32),
        ),
        in_specs=[any_spec] * 6,
        out_specs=(pl.BlockSpec(memory_space=pltpu.VMEM), pl.BlockSpec(memory_space=pltpu.VMEM)),
        scratch_shapes=[
            pltpu.VMEM((2, E_DEV, SAMP), BF16),
            pltpu.SMEM((E_DEV,), jnp.int32),
            pltpu.SMEM((16,), jnp.int32),
            pltpu.VMEM((TAPS, CH), BF16),
            pltpu.VMEM((128, 128), F32),
            pltpu.VMEM((128, 128), F32),
            pltpu.VMEM((128 * PAD, 128), F32),
            pltpu.VMEM((E_DEV, 128), jnp.int32),
            pltpu.VMEM((64, 2 * CH), BF16),
            pltpu.VMEM((128, 2 * CH), BF16),
            pltpu.VMEM((4, 8, 128), BF16),
            pltpu.VMEM((64, 8, 128), BF16),
            pltpu.VMEM((8, 128, 256), BF16),
            pltpu.VMEM((8, 256, 256), BF16),
            pltpu.VMEM((8 * E_DEV, CH), BF16),
            pltpu.VMEM((8, 4, 16384), BF16),
            pltpu.VMEM((128, 128), F32),
            pltpu.VMEM((32, 16384), BF16),
            pltpu.VMEM((RING, RING, 32, 128), BF16),
            pltpu.VMEM((RING, RING, 32, 128), BF16),
            pltpu.VMEM((32, 128), F32),
            pltpu.VMEM((32, 128), F32),
            dma((5,)),
            dma((4,)),
            dma,
            dma((2 * RING,)),
            dma((2, 2, 4)),
            dma((2, 2, 4, RING)),
        ],
        compiler_params=pltpu.CompilerParams(collective_id=0, has_side_effects=True, vmem_limit_bytes=48_000_000),
        name="channelize_and_beamform",
    )(*arrays)
    power, beams = pl.pallas_call(
        put_out,
        out_shape=(jax.ShapeDtypeStruct((E_DEV, CH), BF16), jax.ShapeDtypeStruct((2, 4, 16), F32)),
        in_specs=[pl.BlockSpec(memory_space=pltpu.VMEM)] * 2,
        out_specs=(pl.BlockSpec(memory_space=pltpu.HBM),) * 2,
        scratch_shapes=[dma((2,))],
        compiler_params=pltpu.CompilerParams(vmem_limit_bytes=16_000_000),
        name="put_out",
    )(power, beams)
    beams = jnp.transpose(beams, (0, 2, 1))
    return power, beams


def solution(mesh):
    finer = Mesh(mesh.devices.reshape(8, 2, 8, 2, 2), ("z", "xl", "y", "xh", "core"))
    elem, chan = ("z", "xl", "y"), ("xh", "core")
    placed = (P(None, elem + chan, None), P(elem + chan), P(), P(), P(elem, None, chan, None))
    return jax.shard_map(
        on_device,
        mesh=finer,
        in_specs=placed,
        out_specs=(P(elem + chan, None), P(None, chan, elem)),
        check_vma=False,
    )
```
